64 devices in a mesh: data: 4 (over x, y), sp: 16 (over z, core).
Axes of the slice: x: 2, y: 2, z: 8, core: 2. Of those that a mesh axis runs over, the one named last changes fastest.
The devices are a block of a 4x4x8 slice.
Arguments:
- latents: bfloat16 [8, 48, 256, 384], P('data', 'sp'), parts along dimension 0
- norms: float32 [4, 4, 384], replicated
- w_qkv: bfloat16 [4, 384, 3, 6, 64], replicated
- w_out: bfloat16 [4, 6, 64, 384], replicated
- w_up: bfloat16 [4, 384, 1536], replicated
- w_down: bfloat16 [4, 1536, 384], replicated
Outputs:
- output: bfloat16 [8, 48, 256, 384], P('data', None, 'sp'), parts along dimension 0
There are 4 independent parts. The reference program is written for one: setup_inputs(seed, part) draws one part's arguments, and reference() takes and returns one part's arrays. A program takes and returns all parts, laid end to end along the dimension named above; an argument that names none is the same for every part.
All inputs are finite; a program needn't handle non-finite values.
Results may differ from the reference program's by a relative error of at most 0.0161434.
Values are sent between devices in bfloat16 or wider.
A program may use at most 768 MiB of HBM per device.

```python
import math
import jax
import jax.numpy as jnp
from jax import lax

BATCH = 2
FRAMES = 48
PATCHES = 256
WIDTH = 384
HEADS = 6
BLOCKS = 4
HEAD_DIM = WIDTH // HEADS
HIDDEN = 4 * WIDTH
EPS = 1e-6
SPATIAL = (2, 'btqhe,btkhe->bthqk', 'bthqk,btkhe->btqhe')
TEMPORAL = (1, 'bqshe,bkshe->bshqk', 'bshqk,bkshe->bqshe')


def setup_inputs(seed: int = 0, part: int = 0) -> dict:
    base_key = jax.random.key(seed)
    part_key = jax.random.fold_in(base_key, part)
    time_key, space_key, noise_key = jax.random.split(part_key, 3)
    time_walk = jnp.cumsum(jax.random.normal(time_key, (BATCH, FRAMES, WIDTH), jnp.float32), axis=1) * (1.5 / math.sqrt(FRAMES))
    space_walk = jnp.cumsum(jax.random.normal(space_key, (BATCH, PATCHES, WIDTH), jnp.float32), axis=1) * (1.0 / math.sqrt(PATCHES))
    noise = jax.random.normal(noise_key, (BATCH, FRAMES, PATCHES, WIDTH), jnp.float32)
    latents = (time_walk[:, :, None, :] + space_walk[:, None, :, :] + 0.5 * noise).astype(jnp.bfloat16)
    weight_keys = jax.random.split(jax.random.key(seed + 1), 5)
    norm_base = jnp.array([1.0, 0.0, 1.0, 0.0], jnp.float32)
    norms = norm_base[None, :, None] + 0.3 * jax.random.normal(weight_keys[0], (BLOCKS, 4, WIDTH), jnp.float32)
    qkv_gain = jnp.array([1.2, 1.2, 1.0], jnp.float32)[None, None, :, None, None]
    w_qkv = (jax.random.normal(weight_keys[1], (BLOCKS, WIDTH, 3, HEADS, HEAD_DIM), jnp.float32) * qkv_gain / math.sqrt(WIDTH)).astype(jnp.bfloat16)
    w_out = (jax.random.normal(weight_keys[2], (BLOCKS, HEADS, HEAD_DIM, WIDTH), jnp.float32) / math.sqrt(WIDTH)).astype(jnp.bfloat16)
    w_up = (jax.random.normal(weight_keys[3], (BLOCKS, WIDTH, HIDDEN), jnp.float32) / math.sqrt(WIDTH)).astype(jnp.bfloat16)
    w_down = (jax.random.normal(weight_keys[4], (BLOCKS, HIDDEN, WIDTH), jnp.float32) / math.sqrt(HIDDEN)).astype(jnp.bfloat16)
    return {'latents': latents, 'norms': norms, 'w_qkv': w_qkv, 'w_out': w_out, 'w_up': w_up, 'w_down': w_down}


def layer_norm(tokens, norm_gain, norm_shift):
    tokens_f32 = tokens.astype(jnp.float32)
    row_mean = jnp.mean(tokens_f32, axis=-1, keepdims=True)
    centered = tokens_f32 - row_mean
    variance = jnp.mean(jnp.square(centered), axis=-1, keepdims=True)
    return (centered * lax.rsqrt(variance + EPS) * norm_gain + norm_shift).astype(jnp.bfloat16)


def attention(query_rows, key_rows, value_rows, layout):
    seq_axis, score_form, mix_form = layout
    seq_len = query_rows.shape[seq_axis]
    q_block = math.gcd(seq_len, 64)
    logit_scale = HEAD_DIM ** -0.5
    key_f32 = key_rows.astype(jnp.float32)
    value_f32 = value_rows.astype(jnp.float32)

    def attend_block(block_idx, attn_out):
        q_start = block_idx * q_block
        q_part = lax.dynamic_slice_in_dim(query_rows, q_start, q_block, axis=seq_axis).astype(jnp.float32)
        logits = jnp.einsum(score_form, q_part, key_f32) * logit_scale
        attn_probs = jax.nn.softmax(logits, axis=-1).astype(jnp.bfloat16).astype(jnp.float32)
        block_out = jnp.einsum(mix_form, attn_probs, value_f32).astype(jnp.bfloat16)
        return lax.dynamic_update_slice_in_dim(attn_out, block_out, q_start, axis=seq_axis)

    return lax.fori_loop(0, seq_len // q_block, attend_block, jnp.zeros_like(query_rows))


def project_heads(normed, head_weight):
    return jnp.einsum('btsd,dhe->btshe', normed.astype(jnp.float32), head_weight.astype(jnp.float32)).astype(jnp.bfloat16)


def transformer_block(tokens, norm_rows, qkv_weight, out_weight, up_weight, down_weight, layout):
    normed = layer_norm(tokens, norm_rows[0], norm_rows[1])
    mixed_heads = attention(project_heads(normed, qkv_weight[:, 0]), project_heads(normed, qkv_weight[:, 1]), project_heads(normed, qkv_weight[:, 2]), layout)
    attn_proj = jnp.einsum('btshe,hed->btsd', mixed_heads.astype(jnp.float32), out_weight.astype(jnp.float32))
    residual = (tokens.astype(jnp.float32) + attn_proj).astype(jnp.bfloat16)
    normed_mlp = layer_norm(residual, norm_rows[2], norm_rows[3])
    up_proj = jnp.einsum('btsd,df->btsf', normed_mlp.astype(jnp.float32), up_weight.astype(jnp.float32))
    hidden = jax.nn.gelu(up_proj, approximate=True).astype(jnp.bfloat16)
    down_proj = jnp.einsum('btsf,fd->btsd', hidden.astype(jnp.float32), down_weight.astype(jnp.float32))
    return (residual.astype(jnp.float32) + down_proj).astype(jnp.bfloat16)


def reference(latents, norms, w_qkv, w_out, w_up, w_down):
    tokens = latents
    for layer_idx in range(BLOCKS):
        layout = SPATIAL if layer_idx % 2 == 0 else TEMPORAL
        tokens = transformer_block(tokens, norms[layer_idx], w_qkv[layer_idx], w_out[layer_idx], w_up[layer_idx], w_down[layer_idx], layout)
    return tokens
```

```python
import functools
import math
import jax
import jax.numpy as jnp
from jax import lax
from jax.experimental import pallas as pl
from jax.experimental.pallas import tpu as pltpu
from jax.sharding import PartitionSpec as P

EPS = 1e-6
LANES = 128
MASKED = -1e38
F32, BF16 = jnp.float32, jnp.bfloat16


def dot(a, b):
    return jnp.dot(a, b, preferred_element_type=F32)


def dot_nt(a, b):
    return lax.dot_general(a, b, (((1,), (1,)), ((), ())), preferred_element_type=F32)


def layer_norm(x, gain, shift):
    centered = x - jnp.mean(x, axis=-1, keepdims=True)
    variance = jnp.mean(centered * centered, axis=-1, keepdims=True)
    return centered * lax.rsqrt(variance + EPS) * gain + shift


def kernel(n, head, x_ref, norms, wqkv_hbm, wout_hbm, wup_hbm, wdown_hbm, y_ref,
           wqkv, wout, wup, wdown, s_in, s_out, t_in, t_out, qkv_s, attn_s, hid_s, a_f32, o_f32, mask_s,
           w_sem, x_sem, b_recv, ac_recv, b_send, ac_send, y_sem):
    pairs, videos, f_loc, patches, width = s_in.shape
    frames, p_loc = t_in.shape[2], t_in.shape[3]
    rows_t = frames * p_loc
    me = lax.axis_index("sp")
    pair_heads = width // LANES
    group = 4
    rows_g = group * frames
    scale = head ** -0.5

    barrier = pltpu.get_barrier_semaphore()

    def tell(step, c):
        pl.semaphore_signal(barrier, inc=1, device_id={"sp": lax.rem(me + step, n)})
        return c

    lax.fori_loop(1, n, tell, 0)

    def weight_copies(layer):
        return [pltpu.make_async_copy(src.at[layer], dst.at[layer], w_sem.at[layer, i])
                for i, (src, dst) in enumerate(((wqkv_hbm, wqkv), (wout_hbm, wout), (wup_hbm, wup), (wdown_hbm, wdown)))]

    def start_weights(layer):
        for c in weight_copies(layer):
            c.start()

    for v in range(videos):
        pltpu.make_async_copy(x_ref.at[v], s_in.at[0, v], x_sem.at[v]).start()
    start_weights(0)

    row_p = lax.broadcasted_iota(jnp.int32, (rows_g, rows_g), 0)
    col_p = lax.broadcasted_iota(jnp.int32, (rows_g, rows_g), 1)
    same = jnp.zeros((rows_g, rows_g), F32)
    for i in range(group):
        lo, hi = i * frames, (i + 1) * frames
        inside = (row_p >= lo) & (row_p < hi) & (col_p >= lo) & (col_p < hi)
        same = jnp.where(inside, 1.0, same)
    mask_s[...] = same

    lane = lax.broadcasted_iota(jnp.int32, (1, LANES), 1)
    keep = [jnp.where(lane // head == i, 1.0, 0.0).astype(BF16) for i in range(LANES // head)]

    def project(a, rows, layer):
        qkv_s[pl.ds(0, rows), pl.ds(0, width)] = (dot(a, wqkv[layer, :, pl.ds(0, width)]) * scale).astype(BF16)
        qkv_s[pl.ds(0, rows), pl.ds(width, 2 * width)] = dot(a, wqkv[layer, :, pl.ds(width, 2 * width)]).astype(BF16)

    def attend(rows, masked, put):
        for j in range(pair_heads):
            q = qkv_s[pl.ds(0, rows), pl.ds(j * LANES, LANES)]
            k = qkv_s[pl.ds(0, rows), pl.ds(width + j * LANES, LANES)]
            v = qkv_s[pl.ds(0, rows), pl.ds(2 * width + j * LANES, LANES)]
            out = None
            for i in range(LANES // head):
                s = dot_nt(q, k * keep[i])
                if masked:
                    s = jnp.where(mask_s[...] > 0.5, s, MASKED)
                e = jnp.exp(s - jnp.max(s, axis=-1, keepdims=True))
                p = (e * (1.0 / jnp.sum(e, axis=-1, keepdims=True))).astype(BF16)
                part = dot(p, v * keep[i])
                out = part if out is None else out + part
            put(j, out)

    def finish(u, o, layer, rows):
        h = (u.astype(F32) + dot(o, wout[layer])).astype(BF16)
        hf = h.astype(F32)
        a2 = layer_norm(hf, norms[layer, pl.ds(2, 1), :], norms[layer, pl.ds(3, 1), :]).astype(BF16)
        chunk = 512
        for c in range(hid_s.shape[1] // chunk):
            up = dot(a2, wup[layer, :, pl.ds(c * chunk, chunk)])
            hid_s[pl.ds(0, rows), pl.ds(c * chunk, chunk)] = jax.nn.gelu(up, approximate=True).astype(BF16)
        return (hf + dot(hid_s[pl.ds(0, rows), :], wdown[layer])).astype(BF16)

    def spatial_frame(pair, v, f):
        layer = 2 * pair
        u = s_in[pair, v, f]
        a = layer_norm(u.astype(F32), norms[layer, pl.ds(0, 1), :], norms[layer, pl.ds(1, 1), :]).astype(BF16)
        project(a, patches, layer)

        def put(j, out):
            attn_s[pl.ds(0, patches), pl.ds(j * LANES, LANES)] = out.astype(BF16)

        attend(patches, False, put)
        s_out[pair, v, f] = finish(s_in[pair, v, f], attn_s[...], layer, patches)

    def send_frame(pair, v, f):
        local = pltpu.make_async_copy(s_out.at[pair, v, f, pl.ds(pl.multiple_of(me * p_loc, p_loc), p_loc), :], t_in.at[pair, v, me * f_loc + f], ac_recv.at[pair, v])
        local.start()

        def one(step, c):
            to = lax.rem(me + (n // 2) + step, n)

            pltpu.make_async_remote_copy(
                src_ref=s_out.at[pair, v, f, pl.ds(pl.multiple_of(to * p_loc, p_loc), p_loc), :],
                dst_ref=t_in.at[pair, v, me * f_loc + f],
                send_sem=ac_send.at[pair, v], recv_sem=ac_recv.at[pair, v],
                device_id={"sp": to}).start()
            return c

        def both(i, c):
            one(i, c)

            @pl.when(i > 0)
            def _():
                one(n - i, c)
            return c

        lax.fori_loop(0, n // 2, both, 0)

    def send_chunk(pair, v, to):
        src = t_out.at[pair, v, pl.ds(to * f_loc, f_loc)]
        dst = s_in.at[pair + 1, v, :, pl.ds(pl.multiple_of(me * p_loc, p_loc), p_loc), :]

        @pl.when(to == me)
        def _():
            pltpu.make_async_copy(src, dst, b_recv.at[v]).start()

        @pl.when(to != me)
        def _():
            pltpu.make_async_remote_copy(src_ref=src, dst_ref=dst, send_sem=b_send.at[v], recv_sem=b_recv.at[v], device_id={"sp": to}).start()

    def temporal(pair, v):
        layer = 2 * pair + 1
        f_chunk = frames // 4
        rows_c = f_chunk * p_loc
        to_chunk = f_chunk // f_loc

        def phase1(c, carry):
            u = t_in[pair, v, pl.ds(c * f_chunk, f_chunk)].reshape(rows_c, width).astype(F32)
            a = layer_norm(u, norms[layer, pl.ds(0, 1), :], norms[layer, pl.ds(1, 1), :])
            for j in range(pair_heads):
                a_f32[j, pl.ds(pl.multiple_of(c * rows_c, rows_c), rows_c), :] = a[:, j * LANES:(j + 1) * LANES]
            return carry

        lax.fori_loop(0, 4, phase1, 0)

        def phase2(g, carry):
            for i in range(group):
                for j in range(pair_heads):
                    attn_s[pl.ds(i * frames, frames), pl.ds(j * LANES, LANES)] = a_f32[j, pl.ds(g * group + i, frames, stride=p_loc), :].astype(BF16)
            project(attn_s[pl.ds(0, rows_g), :], rows_g, layer)

            def put(j, out):
                for i in range(group):
                    o_f32[j, pl.ds(g * group + i, frames, stride=p_loc), :] = out[i * frames:(i + 1) * frames]

            attend(rows_g, True, put)
            return carry

        lax.fori_loop(0, p_loc // group, phase2, 0)

        def phase3(i, carry):
            c = lax.rem(me // to_chunk + 2 + 3 * i + 3 * ((i * (i - 1)) // 2), 4)
            rows = pl.ds(pl.multiple_of(c * rows_c, rows_c), rows_c)
            for j in range(pair_heads):
                attn_s[pl.ds(0, rows_c), pl.ds(j * LANES, LANES)] = o_f32[j, rows, :].astype(BF16)
            u = t_in[pair, v, pl.ds(c * f_chunk, f_chunk)].reshape(rows_c, width)
            z = finish(u, attn_s[pl.ds(0, rows_c), :], layer, rows_c)
            t_out[pair, v, pl.ds(c * f_chunk, f_chunk)] = z.reshape(f_chunk, p_loc, width)

            @pl.when(pair < pairs - 1)
            def _():
                lax.fori_loop(0, to_chunk, lambda k, q: (send_chunk(pair, v, c * to_chunk + k), q)[1], 0)

            @pl.when(pair == pairs - 1)
            def _():
                pltpu.make_async_copy(t_out.at[pair, v, pl.ds(c * f_chunk, f_chunk)], y_ref.at[v, pl.ds(c * f_chunk, f_chunk)], y_sem.at[v]).start()
            return carry

        lax.fori_loop(0, 4, phase3, 0)

    def run_pair(pair, carry):
        layer = 2 * pair
        for c in weight_copies(layer):
            c.wait()
        start_weights(layer + 1)
        for v in range(videos):
            @pl.when(pair == 0)
            def _():
                pltpu.make_async_copy(x_ref.at[v], s_in.at[0, v], x_sem.at[v]).wait()

            @pl.when(pair > 0)
            def _():
                pltpu.make_async_copy(x_ref.at[v], s_in.at[1, v], b_recv.at[v]).wait()

            def frame(f, q):
                spatial_frame(pair, v, f)
                if v == 0:
                    @pl.when((f == 0) & (pair == 0))
                    def _():
                        pl.semaphore_wait(barrier, n - 1)
                send_frame(pair, v, f)
                return q

            lax.fori_loop(0, f_loc, frame, 0)
        for c in weight_copies(layer + 1):
            c.wait()

        @pl.when(pair < pairs - 1)
        def _():
            start_weights(layer + 2)

        for v in range(videos):
            pltpu.make_async_copy(t_in.at[pair, v], t_in.at[pair, v], ac_recv.at[pair, v]).wait()
            temporal(pair, v)
        return carry

    lax.fori_loop(0, pairs, run_pair, 0)

    for v in range(videos):
        pltpu.make_async_copy(y_ref.at[v], y_ref.at[v], y_sem.at[v]).wait()
        part = t_in.at[0, v, pl.ds(0, frames - f_loc)]
        for pair in range(pairs):
            pltpu.make_async_copy(part, part, ac_send.at[pair, v]).wait()
        for pair in range(pairs - 1):
            pltpu.make_async_copy(part, part, b_send.at[v]).wait()


def solution(mesh):
    n = mesh.shape["sp"]

    def local_stack(x, norms, w_qkv, w_out, w_up, w_down):
        videos, f_loc, patches, width = x.shape
        layers = w_qkv.shape[0]
        pairs = layers // 2
        head = w_qkv.shape[-1]
        hidden = w_up.shape[-1]
        frames, p_loc = f_loc * n, patches // n
        w_qkv = w_qkv.reshape(layers, width, 3 * width)
        w_out = w_out.reshape(layers, width, width)
        any_space = pl.BlockSpec(memory_space=pl.ANY)
        return pl.pallas_call(
            functools.partial(kernel, n, head),
            out_shape=jax.ShapeDtypeStruct((videos, frames, p_loc, width), BF16),
            in_specs=[any_space, pl.BlockSpec(memory_space=pltpu.VMEM)] + [any_space] * 4,
            out_specs=any_space,
            scratch_shapes=[
                pltpu.VMEM((layers, width, 3 * width), BF16),
                pltpu.VMEM((layers, width, width), BF16),
                pltpu.VMEM((layers, width, hidden), BF16),
                pltpu.VMEM((layers, hidden, width), BF16),
                pltpu.VMEM((pairs, videos, f_loc, patches, width), BF16),
                pltpu.VMEM((pairs, videos, f_loc, patches, width), BF16),
                pltpu.VMEM((pairs, videos, frames, p_loc, width), BF16),
                pltpu.VMEM((pairs, videos, frames, p_loc, width), BF16),
                pltpu.VMEM((patches, 3 * width), BF16),
                pltpu.VMEM((patches, width), BF16),
                pltpu.VMEM((patches, hidden), BF16),
                pltpu.VMEM((width // LANES, frames * p_loc, LANES), F32),
                pltpu.VMEM((width // LANES, frames * p_loc, LANES), F32),
                pltpu.VMEM((4 * frames, 4 * frames), F32),
                pltpu.SemaphoreType.DMA((layers, 4)),
                pltpu.SemaphoreType.DMA((videos,)),
                pltpu.SemaphoreType.DMA((videos,)),
                pltpu.SemaphoreType.DMA((pairs, videos)),
                pltpu.SemaphoreType.DMA((videos,)),
                pltpu.SemaphoreType.DMA((pairs, videos)),
                pltpu.SemaphoreType.DMA((videos,)),
            ],
            compiler_params=pltpu.CompilerParams(collective_id=0, has_side_effects=True, vmem_limit_bytes=60 * 1024 * 1024),
            name="stack",
        )(x, norms, w_qkv, w_out, w_up, w_down)

    replicated = P()
    return jax.shard_map(local_stack, mesh=mesh, in_specs=(P('data', 'sp', None, None), replicated, replicated, replicated, replicated, replicated), out_specs=P('data', None, 'sp', None), check_vma=False)
```

```python
import functools
import math
import jax
import jax.numpy as jnp
from jax import lax
from jax.experimental import pallas as pl
from jax.experimental.pallas import tpu as pltpu
from jax.sharding import PartitionSpec as P

EPS = 1e-6
LANES = 128
MASKED = -1e38
GELU_A, GELU_B = math.sqrt(2 / math.pi), 0.044715
F32, BF16 = jnp.float32, jnp.bfloat16


def dot(a, b):
    return jnp.dot(a, b, preferred_element_type=F32)


def dot_nt(a, b):
    return lax.dot_general(a, b, (((1,), (1,)), ((), ())), preferred_element_type=F32)


def dot_tn(a, b):
    return lax.dot_general(a, b, (((0,), (0,)), ((), ())), preferred_element_type=F32)


def layer_norm(x, gain, shift):
    centered = x - jnp.mean(x, axis=-1, keepdims=True)
    variance = jnp.mean(centered * centered, axis=-1, keepdims=True)
    return centered * lax.rsqrt(variance + EPS) * gain + shift


def kernel(n, head, x_ref, norms, wqkv_hbm, wout_hbm, wup_hbm, wdown_hbm, y_ref,
           wqkv, wout, wup, wdown, s_in, s_out, t_in, t_out, q_s, k_s, v_s, attn_s, ot_s, s_s, hid_s, a_f32, o_f32, mask_s,
           w_sem, x_sem, b_recv, ac_recv, b_send, ac_send, y_sem):
    pairs, videos, f_loc, patches, width = s_in.shape
    frames, p_loc = t_in.shape[2], t_in.shape[3]
    rows_t = frames * p_loc
    me = lax.axis_index("sp")
    pair_heads = width // LANES
    group = 4
    rows_g = group * frames
    scale = head ** -0.5

    barrier = pltpu.get_barrier_semaphore()

    def tell(step, c):
        pl.semaphore_signal(barrier, inc=1, device_id={"sp": lax.rem(me + step, n)})
        return c

    lax.fori_loop(1, n, tell, 0)

    def weight_copies(layer):
        return [pltpu.make_async_copy(src.at[layer], dst.at[layer], w_sem.at[layer, i])
                for i, (src, dst) in enumerate(((wqkv_hbm, wqkv), (wout_hbm, wout), (wup_hbm, wup), (wdown_hbm, wdown)))]

    def start_weights(layer):
        for c in weight_copies(layer):
            c.start()

    for v in range(videos):
        pltpu.make_async_copy(x_ref.at[v], s_in.at[0, v], x_sem.at[v]).start()
    start_weights(0)

    row_p = lax.broadcasted_iota(jnp.int32, (rows_g, rows_g), 0)
    col_p = lax.broadcasted_iota(jnp.int32, (rows_g, rows_g), 1)
    same = jnp.zeros((rows_g, rows_g), F32)
    for i in range(group):
        lo, hi = i * frames, (i + 1) * frames
        inside = (row_p >= lo) & (row_p < hi) & (col_p >= lo) & (col_p < hi)
        same = jnp.where(inside, 1.0, same)
    mask_s[...] = same

    q_s[...] = jnp.zeros_like(q_s)

    def project(a, rows, layer):
        q = (dot_nt(wqkv[layer, pl.ds(0, width), :], a) * scale).astype(BF16)
        for h in range(width // head):
            q_s[h, pl.ds(h * head % LANES, head), pl.ds(0, rows)] = q[h * head:(h + 1) * head]
        k_s[pl.ds(0, rows), :] = dot_nt(a, wqkv[layer, pl.ds(width, width), :]).astype(BF16)
        v_s[:, pl.ds(0, rows)] = dot_nt(wqkv[layer, pl.ds(2 * width, width), :], a).astype(BF16)

    def attend(rows, masked):
        heads = width // head
        spread = math.log(rows)

        def scores(h):
            s = dot(k_s[pl.ds(0, rows), pl.ds(h * head // LANES * LANES, LANES)], q_s[h, :, pl.ds(0, rows)])
            if masked:
                s = jnp.where(mask_s[...] > 0.5, s, MASKED)
            s_s[h % 2, pl.ds(0, rows), pl.ds(0, rows)] = s
            return jnp.max(s, axis=0, keepdims=True) + spread

        def mix(h, top):
            e = jnp.exp(s_s[h % 2, pl.ds(0, rows), pl.ds(0, rows)] - top)
            o = dot(v_s[pl.ds(h * head, head), pl.ds(0, rows)], e.astype(BF16))
            ot_s[pl.ds(h * head, head), pl.ds(0, rows)] = (o * (1.0 / jnp.sum(e, axis=0, keepdims=True))).astype(BF16)

        top = scores(0)
        for h in range(heads):
            later = scores(h + 1) if h + 1 < heads else None
            mix(h, top)
            top = later

    def out_project(rows, layer):
        return dot_tn(ot_s[:, pl.ds(0, rows)], wout[layer])

    def gelu(x):
        t = jnp.tanh(x * (GELU_A + (GELU_A * GELU_B) * (x * x)))
        half = 0.5 * x
        return half + half * t

    def finish(u, o, layer, rows):
        h = (u.astype(F32) + o).astype(BF16)
        hf = h.astype(F32)
        a2 = layer_norm(hf, norms[layer, pl.ds(2, 1), :], norms[layer, pl.ds(3, 1), :]).astype(BF16)
        chunk = 512
        for c in range(hid_s.shape[1] // chunk):
            up = dot(a2, wup[layer, :, pl.ds(c * chunk, chunk)])
            hid_s[pl.ds(0, rows), pl.ds(c * chunk, chunk)] = gelu(up).astype(BF16)
        return (hf + dot(hid_s[pl.ds(0, rows), :], wdown[layer])).astype(BF16)

    def spatial_frame(pair, v, f):
        layer = 2 * pair
        u = s_in[pair, v, f]
        a = layer_norm(u.astype(F32), norms[layer, pl.ds(0, 1), :], norms[layer, pl.ds(1, 1), :]).astype(BF16)
        project(a, patches, layer)

        attend(patches, False)
        s_out[pair, v, f] = finish(s_in[pair, v, f], out_project(patches, layer), layer, patches)

    def send_frame(pair, v, f):
        local = pltpu.make_async_copy(s_out.at[pair, v, f, pl.ds(pl.multiple_of(me * p_loc, p_loc), p_loc), :], t_in.at[pair, v, me * f_loc + f], ac_recv.at[pair, v])
        local.start()

        def one(step, c):
            to = lax.rem(me + (n // 2) + step, n)

            pltpu.make_async_remote_copy(
                src_ref=s_out.at[pair, v, f, pl.ds(pl.multiple_of(to * p_loc, p_loc), p_loc), :],
                dst_ref=t_in.at[pair, v, me * f_loc + f],
                send_sem=ac_send.at[pair, v], recv_sem=ac_recv.at[pair, v],
                device_id={"sp": to}).start()
            return c

        def both(i, c):
            one(i, c)

            @pl.when(i > 0)
            def _():
                one(n - i, c)
            return c

        lax.fori_loop(0, n // 2, both, 0)

    def send_chunk(pair, v, to):
        src = t_out.at[pair, v, pl.ds(to * f_loc, f_loc)]
        dst = s_in.at[pair + 1, v, :, pl.ds(pl.multiple_of(me * p_loc, p_loc), p_loc), :]

        @pl.when(to == me)
        def _():
            pltpu.make_async_copy(src, dst, b_recv.at[v]).start()

        @pl.when(to != me)
        def _():
            pltpu.make_async_remote_copy(src_ref=src, dst_ref=dst, send_sem=b_send.at[v], recv_sem=b_recv.at[v], device_id={"sp": to}).start()

    def temporal(pair, v):
        layer = 2 * pair + 1
        f_chunk = frames // 4
        rows_c = f_chunk * p_loc
        to_chunk = f_chunk // f_loc

        def phase1(c, carry):
            u = t_in[pair, v, pl.ds(c * f_chunk, f_chunk)].reshape(rows_c, width).astype(F32)
            a = layer_norm(u, norms[layer, pl.ds(0, 1), :], norms[layer, pl.ds(1, 1), :])
            for j in range(pair_heads):
                a_f32[j, pl.ds(pl.multiple_of(c * rows_c, rows_c), rows_c), :] = a[:, j * LANES:(j + 1) * LANES]
            return carry

        lax.fori_loop(0, 4, phase1, 0)

        def phase2(g, carry):
            for i in range(group):
                for j in range(pair_heads):
                    attn_s[pl.ds(i * frames, frames), pl.ds(j * LANES, LANES)] = a_f32[j, pl.ds(g * group + i, frames, stride=p_loc), :].astype(BF16)
            project(attn_s[pl.ds(0, rows_g), :], rows_g, layer)

            attend(rows_g, True)
            o = out_project(rows_g, layer)
            for i in range(group):
                for j in range(pair_heads):
                    o_f32[j, pl.ds(g * group + i, frames, stride=p_loc), :] = o[i * frames:(i + 1) * frames, j * LANES:(j + 1) * LANES]
            return carry

        lax.fori_loop(0, p_loc // group, phase2, 0)

        def phase3(i, carry):
            c = lax.rem(me // to_chunk + 2 + 3 * i + 3 * ((i * (i - 1)) // 2), 4)
            rows = pl.ds(pl.multiple_of(c * rows_c, rows_c), rows_c)
            o = jnp.concatenate([o_f32[j, rows, :] for j in range(pair_heads)], axis=1)
            u = t_in[pair, v, pl.ds(c * f_chunk, f_chunk)].reshape(rows_c, width)
            z = finish(u, o, layer, rows_c)
            t_out[pair, v, pl.ds(c * f_chunk, f_chunk)] = z.reshape(f_chunk, p_loc, width)

            @pl.when(pair < pairs - 1)
            def _():
                lax.fori_loop(0, to_chunk, lambda k, q: (send_chunk(pair, v, c * to_chunk + k), q)[1], 0)

            @pl.when(pair == pairs - 1)
            def _():
                pltpu.make_async_copy(t_out.at[pair, v, pl.ds(c * f_chunk, f_chunk)], y_ref.at[v, pl.ds(c * f_chunk, f_chunk)], y_sem.at[v]).start()
            return carry

        lax.fori_loop(0, 4, phase3, 0)

    def run_pair(pair, carry):
        layer = 2 * pair
        for c in weight_copies(layer):
            c.wait()
        start_weights(layer + 1)
        for v in range(videos):
            @pl.when(pair == 0)
            def _():
                pltpu.make_async_copy(x_ref.at[v], s_in.at[0, v], x_sem.at[v]).wait()

            @pl.when(pair > 0)
            def _():
                pltpu.make_async_copy(x_ref.at[v], s_in.at[1, v], b_recv.at[v]).wait()

            def frame(f, q):
                spatial_frame(pair, v, f)
                if v == 0:
                    @pl.when((f == 0) & (pair == 0))
                    def _():
                        pl.semaphore_wait(barrier, n - 1)
                send_frame(pair, v, f)
                return q

            lax.fori_loop(0, f_loc, frame, 0)
        for c in weight_copies(layer + 1):
            c.wait()

        @pl.when(pair < pairs - 1)
        def _():
            start_weights(layer + 2)

        for v in range(videos):
            pltpu.make_async_copy(t_in.at[pair, v], t_in.at[pair, v], ac_recv.at[pair, v]).wait()
            temporal(pair, v)
        return carry

    lax.fori_loop(0, pairs, run_pair, 0)

    for v in range(videos):
        pltpu.make_async_copy(y_ref.at[v], y_ref.at[v], y_sem.at[v]).wait()
        part = t_in.at[0, v, pl.ds(0, frames - f_loc)]
        for pair in range(pairs):
            pltpu.make_async_copy(part, part, ac_send.at[pair, v]).wait()
        for pair in range(pairs - 1):
            pltpu.make_async_copy(part, part, b_send.at[v]).wait()


def solution(mesh):
    n = mesh.shape["sp"]

    def local_stack(x, norms, w_qkv, w_out, w_up, w_down):
        videos, f_loc, patches, width = x.shape
        layers = w_qkv.shape[0]
        pairs = layers // 2
        head = w_qkv.shape[-1]
        hidden = w_up.shape[-1]
        frames, p_loc = f_loc * n, patches // n
        w_qkv = w_qkv.transpose(0, 2, 3, 4, 1).reshape(layers, 3 * width, width)
        w_out = w_out.reshape(layers, width, width)
        any_space = pl.BlockSpec(memory_space=pl.ANY)
        return pl.pallas_call(
            functools.partial(kernel, n, head),
            out_shape=jax.ShapeDtypeStruct((videos, frames, p_loc, width), BF16),
            in_specs=[any_space, pl.BlockSpec(memory_space=pltpu.VMEM)] + [any_space] * 4,
            out_specs=any_space,
            scratch_shapes=[
                pltpu.VMEM((layers, 3 * width, width), BF16),
                pltpu.VMEM((layers, width, width), BF16),
                pltpu.VMEM((layers, width, hidden), BF16),
                pltpu.VMEM((layers, hidden, width), BF16),
                pltpu.VMEM((pairs, videos, f_loc, patches, width), BF16),
                pltpu.VMEM((pairs, videos, f_loc, patches, width), BF16),
                pltpu.VMEM((pairs, videos, frames, p_loc, width), BF16),
                pltpu.VMEM((pairs, videos, frames, p_loc, width), BF16),
                pltpu.VMEM((width // head, LANES, patches), BF16),
                pltpu.VMEM((patches, width), BF16),
                pltpu.VMEM((width, patches), BF16),
                pltpu.VMEM((patches, width), BF16),
                pltpu.VMEM((width, patches), BF16),
                pltpu.VMEM((2, patches, patches), F32),
                pltpu.VMEM((patches, hidden), BF16),
                pltpu.VMEM((width // LANES, frames * p_loc, LANES), F32),
                pltpu.VMEM((width // LANES, frames * p_loc, LANES), F32),
                pltpu.VMEM((4 * frames, 4 * frames), F32),
                pltpu.SemaphoreType.DMA((layers, 4)),
                pltpu.SemaphoreType.DMA((videos,)),
                pltpu.SemaphoreType.DMA((videos,)),
                pltpu.SemaphoreType.DMA((pairs, videos)),
                pltpu.SemaphoreType.DMA((videos,)),
                pltpu.SemaphoreType.DMA((pairs, videos)),
                pltpu.SemaphoreType.DMA((videos,)),
            ],
            compiler_params=pltpu.CompilerParams(collective_id=0, has_side_effects=True, vmem_limit_bytes=60 * 1024 * 1024),
            name="stack",
        )(x, norms, w_qkv, w_out, w_up, w_down)

    replicated = P()
    return jax.shard_map(local_stack, mesh=mesh, in_specs=(P('data', 'sp', None, None), replicated, replicated, replicated, replicated, replicated), out_specs=P('data', None, 'sp', None), check_vma=False)
```

```python
import functools
import math
import jax
import jax.numpy as jnp
from jax import lax
from jax.experimental import pallas as pl
from jax.experimental.pallas import tpu as pltpu
from jax.sharding import PartitionSpec as P

EPS = 1e-6
LANES = 128
SUB = 8
MASKED = -1e38
GELU_A, GELU_B = math.sqrt(2 / math.pi), 0.044715
F32, BF16 = jnp.float32, jnp.bfloat16


def dot(a, b):
    return jnp.dot(a, b, preferred_element_type=F32)


def dot_nt(a, b):
    return lax.dot_general(a, b, (((1,), (1,)), ((), ())), preferred_element_type=F32)


def dot_tn(a, b):
    return lax.dot_general(a, b, (((0,), (0,)), ((), ())), preferred_element_type=F32)


def layer_norm(x, gain, shift):
    centered = x - jnp.mean(x, axis=-1, keepdims=True)
    variance = jnp.mean(centered * centered, axis=-1, keepdims=True)
    return centered * lax.rsqrt(variance + EPS) * gain + shift


def kernel(n, head, x_ref, norms, wqkv_hbm, wout_hbm, wup_hbm, wdown_hbm, y_ref,
           wqkv, wout, wup, wdown, s_in, s_out, t_in, t_out, q_s, k_s, v_s, attn_s, ot_s, s_s, hid_s, a_f32, o_f32, mask_s,
           w_sem, x_sem, b_recv, ac_recv, b_send, ac_send, y_sem):
    pairs, videos, f_loc, tiles, sub, width = s_in.shape
    halves, frames = t_in.shape[2], t_in.shape[3]
    patches = tiles * sub
    me = lax.axis_index("sp")
    pair_heads = width // LANES
    group = 4
    rows_g = group * frames
    scale = head ** -0.5

    barrier = pltpu.get_barrier_semaphore()

    def tell(step, c):
        pl.semaphore_signal(barrier, inc=1, device_id={"sp": lax.rem(me + step, n)})
        return c

    lax.fori_loop(1, n, tell, 0)

    def weight_copies(layer):
        return [pltpu.make_async_copy(src.at[layer], dst.at[layer], w_sem.at[layer, i])
                for i, (src, dst) in enumerate(((wqkv_hbm, wqkv), (wout_hbm, wout), (wup_hbm, wup), (wdown_hbm, wdown)))]

    def start_weights(layer):
        for c in weight_copies(layer):
            c.start()

    for v in range(videos):
        pltpu.make_async_copy(x_ref.at[v], s_in.at[0, v], x_sem.at[v]).start()
    start_weights(0)

    row_p = lax.broadcasted_iota(jnp.int32, (rows_g, rows_g), 0)
    col_p = lax.broadcasted_iota(jnp.int32, (rows_g, rows_g), 1)
    same = jnp.zeros((rows_g, rows_g), F32)
    for i in range(group):
        lo, hi = i * frames, (i + 1) * frames
        inside = (row_p >= lo) & (row_p < hi) & (col_p >= lo) & (col_p < hi)
        same = jnp.where(inside, 1.0, same)
    mask_s[...] = same

    q_s[...] = jnp.zeros_like(q_s)

    def project(a, rows, layer):
        q = (dot_nt(wqkv[layer, pl.ds(0, width), :], a) * scale).astype(BF16)
        for h in range(width // head):
            q_s[h, pl.ds(h * head % LANES, head), pl.ds(0, rows)] = q[h * head:(h + 1) * head]
        k_s[pl.ds(0, rows), :] = dot_nt(a, wqkv[layer, pl.ds(width, width), :]).astype(BF16)
        v_s[:, pl.ds(0, rows)] = dot_nt(wqkv[layer, pl.ds(2 * width, width), :], a).astype(BF16)

    def attend(rows, masked):
        heads = width // head
        shift = math.log(rows)

        def scores(h):
            s = dot(k_s[pl.ds(0, rows), pl.ds(h * head // LANES * LANES, LANES)], q_s[h, :, pl.ds(0, rows)])
            if masked:
                s = jnp.where(mask_s[...] > 0.5, s, MASKED)
            s_s[h % 2, pl.ds(0, rows), pl.ds(0, rows)] = s
            return jnp.max(s, axis=0, keepdims=True) + shift

        def mix(h, top):
            e = jnp.exp(s_s[h % 2, pl.ds(0, rows), pl.ds(0, rows)] - top)
            o = dot(v_s[pl.ds(h * head, head), pl.ds(0, rows)], e.astype(BF16))
            ot_s[pl.ds(h * head, head), pl.ds(0, rows)] = (o * (1.0 / jnp.sum(e, axis=0, keepdims=True))).astype(BF16)

        top = scores(0)
        for h in range(heads):
            later = scores(h + 1) if h + 1 < heads else None
            mix(h, top)
            top = later

    def out_project(rows, layer):
        return dot_tn(ot_s[:, pl.ds(0, rows)], wout[layer])

    def gelu(x):
        t = jnp.tanh(x * (GELU_A + (GELU_A * GELU_B) * (x * x)))
        half = 0.5 * x
        return half + half * t

    def finish(u, o, layer, rows):
        h = (u + o).astype(BF16)
        hf = h.astype(F32)
        a2 = layer_norm(hf, norms[layer, pl.ds(2, 1), :], norms[layer, pl.ds(3, 1), :]).astype(BF16)
        chunk = 512
        for c in range(hid_s.shape[1] // chunk):
            up = dot(a2, wup[layer, :, pl.ds(c * chunk, chunk)])
            hid_s[pl.ds(0, rows), pl.ds(c * chunk, chunk)] = gelu(up).astype(BF16)
        return hf + dot(hid_s[pl.ds(0, rows), :], wdown[layer])

    def spatial_frame(pair, v, f):
        layer = 2 * pair
        u = s_in[pair, v, f].astype(F32).reshape(patches, width)
        a = layer_norm(u, norms[layer, pl.ds(0, 1), :], norms[layer, pl.ds(1, 1), :]).astype(BF16)
        project(a, patches, layer)

        attend(patches, False)
        u = s_in[pair, v, f].astype(F32).reshape(patches, width)
        s_out[pair, v, f] = finish(u, out_project(patches, layer), layer, patches).reshape(tiles, sub, width).astype(BF16)

    def spread(send):
        def both(i, c):
            send(lax.rem(me + n // 2 + i, n))

            @pl.when(i > 0)
            def _():
                send(lax.rem(me + n // 2 + n - i, n))
            return c

        lax.fori_loop(0, n // 2, both, 0)

    def send_frame(pair, v, f):
        def part(to):
            return s_out.at[pair, v, f, pl.ds(to * halves, halves)], t_in.at[pair, v, :, me * f_loc + f]

        def send(to):
            src, dst = part(to)
            pltpu.make_async_remote_copy(src_ref=src, dst_ref=dst, send_sem=ac_send.at[pair, v, 0], recv_sem=ac_recv.at[pair, v, 0], device_id={"sp": to}).start()

        src, dst = part(me)
        pltpu.make_async_copy(src, dst, ac_recv.at[pair, v, 0]).start()
        spread(send)

    def send_half(pair, v, h):
        def part(to):
            return s_out.at[pair, v, :, to * halves + h], t_in.at[pair, v, h, pl.ds(me * f_loc, f_loc)]

        def send(to):
            src, dst = part(to)
            pltpu.make_async_remote_copy(src_ref=src, dst_ref=dst, send_sem=ac_send.at[pair, v, h], recv_sem=ac_recv.at[pair, v, h], device_id={"sp": to}).start()

        src, dst = part(me)
        pltpu.make_async_copy(src, dst, ac_recv.at[pair, v, h]).start()
        spread(send)

    def send_chunk(pair, v, h, to):
        src = t_out.at[v, h, pl.ds(to * f_loc, f_loc)]
        dst = s_in.at[pair + 1, v, :, me * halves + h]

        @pl.when(to == me)
        def _():
            pltpu.make_async_copy(src, dst, b_recv.at[v]).start()

        @pl.when(to != me)
        def _():
            pltpu.make_async_remote_copy(src_ref=src, dst_ref=dst, send_sem=b_send.at[v, h], recv_sem=b_recv.at[v], device_id={"sp": to}).start()

    def temporal(pair, v, h):
        layer = 2 * pair + 1
        chunks = 2
        f_chunk = frames // chunks
        rows_c = f_chunk * sub
        to_chunk = f_chunk // f_loc

        def phase1(c, carry):
            u = t_in[pair, v, h, pl.ds(c * f_chunk, f_chunk)].astype(F32).reshape(rows_c, width)
            a = layer_norm(u, norms[layer, pl.ds(0, 1), :], norms[layer, pl.ds(1, 1), :])
            for j in range(pair_heads):
                a_f32[j, pl.ds(pl.multiple_of(c * rows_c, rows_c), rows_c), :] = a[:, j * LANES:(j + 1) * LANES]
            return carry

        lax.fori_loop(0, chunks, phase1, 0)

        def phase2(g, carry):
            for i in range(group):
                for j in range(pair_heads):
                    attn_s[pl.ds(i * frames, frames), pl.ds(j * LANES, LANES)] = a_f32[j, pl.ds(g * group + i, frames, stride=sub), :].astype(BF16)
            project(attn_s[pl.ds(0, rows_g), :], rows_g, layer)
            attend(rows_g, True)
            o = out_project(rows_g, layer)
            for i in range(group):
                for j in range(pair_heads):
                    o_f32[j, pl.ds(g * group + i, frames, stride=sub), :] = o[i * frames:(i + 1) * frames, j * LANES:(j + 1) * LANES]
            return carry

        lax.fori_loop(0, sub // group, phase2, 0)

        def phase3(i, carry):
            c = lax.rem(me // to_chunk + 1 + i, chunks)
            rows = pl.ds(pl.multiple_of(c * rows_c, rows_c), rows_c)
            o = jnp.concatenate([o_f32[j, rows, :] for j in range(pair_heads)], axis=1)
            u = t_in[pair, v, h, pl.ds(c * f_chunk, f_chunk)].astype(F32).reshape(rows_c, width)
            z = finish(u, o, layer, rows_c)
            t_out[v, h, pl.ds(c * f_chunk, f_chunk)] = z.reshape(f_chunk, sub, width).astype(BF16)

            @pl.when(pair < pairs - 1)
            def _():
                lax.fori_loop(0, to_chunk, lambda k, q: (send_chunk(pair, v, h, c * to_chunk + k), q)[1], 0)

            @pl.when(pair == pairs - 1)
            def _():
                pltpu.make_async_copy(t_out.at[v, h, pl.ds(c * f_chunk, f_chunk)], y_ref.at[v, pl.ds(c * f_chunk, f_chunk), h], y_sem.at[v, h]).start()
            return carry

        @pl.when(pair > 0)
        def _():
            part = t_out.at[v, h, pl.ds(0, frames - f_loc)]
            pltpu.make_async_copy(part, part, b_send.at[v, h]).wait()

        lax.fori_loop(0, chunks, phase3, 0)

    def run_pair(pair, carry):
        layer = 2 * pair
        for c in weight_copies(layer):
            c.wait()
        start_weights(layer + 1)
        for v in range(videos):
            @pl.when(pair == 0)
            def _():
                pltpu.make_async_copy(x_ref.at[v], s_in.at[0, v], x_sem.at[v]).wait()

            @pl.when(pair > 0)
            def _():
                pltpu.make_async_copy(x_ref.at[v], s_in.at[1, v], b_recv.at[v]).wait()

            def frame(f, q):
                spatial_frame(pair, v, f)
                if v == 0:
                    @pl.when((f == 0) & (pair == 0))
                    def _():
                        pl.semaphore_wait(barrier, n - 1)
                    send_frame(pair, v, f)
                return q

            lax.fori_loop(0, f_loc, frame, 0)
            if v > 0:
                for h in range(halves):
                    send_half(pair, v, h)
        for c in weight_copies(layer + 1):
            c.wait()

        @pl.when(pair < pairs - 1)
        def _():
            start_weights(layer + 2)

        for v in range(videos):
            if v == 0:
                pltpu.make_async_copy(t_in.at[pair, v], t_in.at[pair, v], ac_recv.at[pair, v, 0]).wait()

            def half(h, q):
                if v > 0:
                    pltpu.make_async_copy(t_in.at[pair, v, h], t_in.at[pair, v, h], ac_recv.at[pair, v, h]).wait()
                temporal(pair, v, h)
                return q

            lax.fori_loop(0, halves, half, 0)
        return carry

    lax.fori_loop(0, pairs, run_pair, 0)

    for v in range(videos):
        for h in range(halves):
            done = y_ref.at[v, :, h]
            pltpu.make_async_copy(done, done, y_sem.at[v, h]).wait()
            for pair in range(pairs):
                part = t_in.at[pair, v, h, pl.ds(0, frames - f_loc)]
                pltpu.make_async_copy(part, part, ac_send.at[pair, v, h if v else 0]).wait()


def solution(mesh):
    n = mesh.shape["sp"]

    def local_stack(x, norms, w_qkv, w_out, w_up, w_down):
        videos, f_loc, patches, width = x.shape
        layers = w_qkv.shape[0]
        pairs = layers // 2
        head = w_qkv.shape[-1]
        hidden = w_up.shape[-1]
        frames, halves = f_loc * n, patches // n // SUB
        x = x.reshape(videos, f_loc, patches // SUB, SUB, width)
        w_qkv = w_qkv.transpose(0, 2, 3, 4, 1).reshape(layers, 3 * width, width)
        w_out = w_out.reshape(layers, width, width)
        any_space = pl.BlockSpec(memory_space=pl.ANY)
        y = pl.pallas_call(
            functools.partial(kernel, n, head),
            out_shape=jax.ShapeDtypeStruct((videos, frames, halves, SUB, width), BF16),
            in_specs=[any_space, pl.BlockSpec(memory_space=pltpu.VMEM)] + [any_space] * 4,
            out_specs=any_space,
            scratch_shapes=[
                pltpu.VMEM((layers, 3 * width, width), BF16),
                pltpu.VMEM((layers, width, width), BF16),
                pltpu.VMEM((layers, width, hidden), BF16),
                pltpu.VMEM((layers, hidden, width), BF16),
                pltpu.VMEM((pairs, videos, f_loc, patches // SUB, SUB, width), BF16),
                pltpu.VMEM((pairs, videos, f_loc, patches // SUB, SUB, width), BF16),
                pltpu.VMEM((pairs, videos, halves, frames, SUB, width), BF16),
                pltpu.VMEM((videos, halves, frames, SUB, width), BF16),
                pltpu.VMEM((width // head, LANES, patches), BF16),
                pltpu.VMEM((patches, width), BF16),
                pltpu.VMEM((width, patches), BF16),
                pltpu.VMEM((patches, width), BF16),
                pltpu.VMEM((width, patches), BF16),
                pltpu.VMEM((2, patches, patches), F32),
                pltpu.VMEM((patches, hidden), BF16),
                pltpu.VMEM((width // LANES, frames * SUB, LANES), F32),
                pltpu.VMEM((width // LANES, frames * SUB, LANES), F32),
                pltpu.VMEM((4 * frames, 4 * frames), F32),
                pltpu.SemaphoreType.DMA((layers, 4)),
                pltpu.SemaphoreType.DMA((videos,)),
                pltpu.SemaphoreType.DMA((videos,)),
                pltpu.SemaphoreType.DMA((pairs, videos, halves)),
                pltpu.SemaphoreType.DMA((videos, halves)),
                pltpu.SemaphoreType.DMA((pairs, videos, halves)),
                pltpu.SemaphoreType.DMA((videos, halves)),
            ],
            compiler_params=pltpu.CompilerParams(collective_id=0, has_side_effects=True, vmem_limit_bytes=60 * 1024 * 1024),
            name="stack",
        )(x, norms, w_qkv, w_out, w_up, w_down)
        return y.reshape(videos, frames, halves * SUB, width)

    replicated = P()
    return jax.shard_map(local_stack, mesh=mesh, in_specs=(P('data', 'sp', None, None), replicated, replicated, replicated, replicated, replicated), out_specs=P('data', None, 'sp', None), check_vma=False)
```

```python
import functools
import math
import jax
import jax.numpy as jnp
from jax import lax
from jax.experimental import pallas as pl
from jax.experimental.pallas import tpu as pltpu
from jax.sharding import PartitionSpec as P

EPS = 1e-6
LANES = 128
SUB = 8
MASKED = -1e38
GELU_A, GELU_B = math.sqrt(2 / math.pi), 0.044715
F32, BF16 = jnp.float32, jnp.bfloat16


def dot(a, b):
    return jnp.dot(a, b, preferred_element_type=F32)


def dot_nt(a, b):
    return lax.dot_general(a, b, (((1,), (1,)), ((), ())), preferred_element_type=F32)


def dot_tn(a, b):
    return lax.dot_general(a, b, (((0,), (0,)), ((), ())), preferred_element_type=F32)


def layer_norm(x, gain, shift):
    centered = x - jnp.mean(x, axis=-1, keepdims=True)
    variance = jnp.mean(centered * centered, axis=-1, keepdims=True)
    return centered * lax.rsqrt(variance + EPS) * gain + shift


def kernel(n, head, x_ref, norms, wqkv_hbm, wout_hbm, wup_hbm, wdown_hbm, y_ref,
           wqkv, wout, wup, wdown, s_in, s_out, t_in, t_out, q_s, k_s, v_s, attn_s, ot_s, s_s, p_s, hid_s, a_f32, o_f32, mask_s,
           w_sem, x_sem, b_recv, ac_recv, b_send, ac_send, y_sem):
    pairs, videos, f_loc, tiles, sub, width = s_in.shape
    halves, frames = t_in.shape[2], t_in.shape[3]
    patches = tiles * sub
    me = lax.axis_index("sp")
    pair_heads = width // LANES
    group = 4
    rows_g = group * frames
    scale = head ** -0.5

    barrier = pltpu.get_barrier_semaphore()

    def tell(step, c):
        pl.semaphore_signal(barrier, inc=1, device_id={"sp": lax.rem(me + step, n)})
        return c

    lax.fori_loop(1, n, tell, 0)

    def weight_copies(layer):
        return [pltpu.make_async_copy(src.at[layer], dst.at[layer], w_sem.at[layer, i])
                for i, (src, dst) in enumerate(((wqkv_hbm, wqkv), (wout_hbm, wout), (wup_hbm, wup), (wdown_hbm, wdown)))]

    def start_weights(layer):
        for c in weight_copies(layer):
            c.start()

    for v in range(videos):
        pltpu.make_async_copy(x_ref.at[v], s_in.at[0, v], x_sem.at[v]).start()
    start_weights(0)

    row_p = lax.broadcasted_iota(jnp.int32, (rows_g, rows_g), 0)
    col_p = lax.broadcasted_iota(jnp.int32, (rows_g, rows_g), 1)
    same = jnp.zeros((rows_g, rows_g), F32)
    for i in range(group):
        lo, hi = i * frames, (i + 1) * frames
        inside = (row_p >= lo) & (row_p < hi) & (col_p >= lo) & (col_p < hi)
        same = jnp.where(inside, 1.0, same)
    mask_s[...] = same

    q_s[...] = jnp.zeros_like(q_s)

    def project(a, rows, layer):
        q = (dot_nt(wqkv[layer, pl.ds(0, width), :], a) * scale).astype(BF16)
        for h in range(width // head):
            q_s[h, pl.ds(h * head % LANES, head), pl.ds(0, rows)] = q[h * head:(h + 1) * head]
        k_s[pl.ds(0, rows), :] = dot_nt(a, wqkv[layer, pl.ds(width, width), :]).astype(BF16)
        v_s[:, pl.ds(0, rows)] = dot_nt(wqkv[layer, pl.ds(2 * width, width), :], a).astype(BF16)

    def attend(rows, masked):
        heads = width // head
        shift = math.log(rows)

        def scores(h):
            s = dot(k_s[pl.ds(0, rows), pl.ds(h * head // LANES * LANES, LANES)], q_s[h, :, pl.ds(0, rows)])
            if masked:
                s = jnp.where(mask_s[...] > 0.5, s, MASKED)
            s_s[h, pl.ds(0, rows), pl.ds(0, rows)] = s
            return jnp.max(s, axis=0, keepdims=True) + shift

        def weigh(h, top):
            e = jnp.exp(s_s[h, pl.ds(0, rows), pl.ds(0, rows)] - top)
            p_s[h, pl.ds(0, rows), pl.ds(0, rows)] = e.astype(BF16)
            return 1.0 / jnp.sum(e, axis=0, keepdims=True)

        def mix(h, norm):
            o = dot(v_s[pl.ds(h * head, head), pl.ds(0, rows)], p_s[h, pl.ds(0, rows), pl.ds(0, rows)])
            ot_s[pl.ds(h * head, head), pl.ds(0, rows)] = (o * norm).astype(BF16)

        tops = [scores(h) for h in range(heads)]
        norm = [weigh(h, tops[h]) for h in range(heads)]
        for h in range(heads):
            mix(h, norm[h])

    def out_project(rows, layer):
        return dot_tn(ot_s[:, pl.ds(0, rows)], wout[layer])

    def gelu(x):
        t = jnp.tanh(x * (GELU_A + (GELU_A * GELU_B) * (x * x)))
        half = 0.5 * x
        return half + half * t

    def finish(u, o, layer, rows):
        h = (u + o).astype(BF16)
        hf = h.astype(F32)
        a2 = layer_norm(hf, norms[layer, pl.ds(2, 1), :], norms[layer, pl.ds(3, 1), :]).astype(BF16)
        chunk = 512
        for c in range(hid_s.shape[1] // chunk):
            up = dot(a2, wup[layer, :, pl.ds(c * chunk, chunk)])
            hid_s[pl.ds(0, rows), pl.ds(c * chunk, chunk)] = gelu(up).astype(BF16)
        return hf + dot(hid_s[pl.ds(0, rows), :], wdown[layer])

    def spatial_frame(pair, v, f):
        layer = 2 * pair
        u = s_in[pair, v, f].astype(F32).reshape(patches, width)
        a = layer_norm(u, norms[layer, pl.ds(0, 1), :], norms[layer, pl.ds(1, 1), :]).astype(BF16)
        project(a, patches, layer)

        attend(patches, False)
        u = s_in[pair, v, f].astype(F32).reshape(patches, width)
        s_out[pair, v, f] = finish(u, out_project(patches, layer), layer, patches).reshape(tiles, sub, width).astype(BF16)

    def spread(send):
        def both(i, c):
            send(lax.rem(me + n // 2 + i, n))

            @pl.when(i > 0)
            def _():
                send(lax.rem(me + n // 2 + n - i, n))
            return c

        lax.fori_loop(0, n // 2, both, 0)

    def send_frame(pair, v, f):
        def part(to):
            return s_out.at[pair, v, f, pl.ds(to * halves, halves)], t_in.at[pair, v, :, me * f_loc + f]

        def send(to):
            src, dst = part(to)
            pltpu.make_async_remote_copy(src_ref=src, dst_ref=dst, send_sem=ac_send.at[pair, v, 0], recv_sem=ac_recv.at[pair, v, 0], device_id={"sp": to}).start()

        src, dst = part(me)
        pltpu.make_async_copy(src, dst, ac_recv.at[pair, v, 0]).start()
        spread(send)

    def send_half(pair, v, h):
        def part(to):
            return s_out.at[pair, v, :, to * halves + h], t_in.at[pair, v, h, pl.ds(me * f_loc, f_loc)]

        def send(to):
            src, dst = part(to)
            pltpu.make_async_remote_copy(src_ref=src, dst_ref=dst, send_sem=ac_send.at[pair, v, h], recv_sem=ac_recv.at[pair, v, h], device_id={"sp": to}).start()

        src, dst = part(me)
        pltpu.make_async_copy(src, dst, ac_recv.at[pair, v, h]).start()
        spread(send)

    def send_chunk(pair, v, h, to):
        src = t_out.at[v, h, pl.ds(to * f_loc, f_loc)]
        dst = s_in.at[pair + 1, v, :, me * halves + h]

        @pl.when(to == me)
        def _():
            pltpu.make_async_copy(src, dst, b_recv.at[v]).start()

        @pl.when(to != me)
        def _():
            pltpu.make_async_remote_copy(src_ref=src, dst_ref=dst, send_sem=b_send.at[v, h], recv_sem=b_recv.at[v], device_id={"sp": to}).start()

    def temporal(pair, v, h):
        layer = 2 * pair + 1
        chunks = 2
        f_chunk = frames // chunks
        rows_c = f_chunk * sub
        to_chunk = f_chunk // f_loc

        def phase1(c, carry):
            u = t_in[pair, v, h, pl.ds(c * f_chunk, f_chunk)].astype(F32).reshape(rows_c, width)
            a = layer_norm(u, norms[layer, pl.ds(0, 1), :], norms[layer, pl.ds(1, 1), :])
            for j in range(pair_heads):
                a_f32[j, pl.ds(pl.multiple_of(c * rows_c, rows_c), rows_c), :] = a[:, j * LANES:(j + 1) * LANES]
            return carry

        lax.fori_loop(0, chunks, phase1, 0)

        def phase2(g, carry):
            for i in range(group):
                for j in range(pair_heads):
                    attn_s[pl.ds(i * frames, frames), pl.ds(j * LANES, LANES)] = a_f32[j, pl.ds(g * group + i, frames, stride=sub), :].astype(BF16)
            project(attn_s[pl.ds(0, rows_g), :], rows_g, layer)
            attend(rows_g, True)
            o = out_project(rows_g, layer)
            for i in range(group):
                for j in range(pair_heads):
                    o_f32[j, pl.ds(g * group + i, frames, stride=sub), :] = o[i * frames:(i + 1) * frames, j * LANES:(j + 1) * LANES]
            return carry

        lax.fori_loop(0, sub // group, phase2, 0)

        def phase3(i, carry):
            c = lax.rem(me // to_chunk + 1 + i, chunks)
            rows = pl.ds(pl.multiple_of(c * rows_c, rows_c), rows_c)
            o = jnp.concatenate([o_f32[j, rows, :] for j in range(pair_heads)], axis=1)
            u = t_in[pair, v, h, pl.ds(c * f_chunk, f_chunk)].astype(F32).reshape(rows_c, width)
            z = finish(u, o, layer, rows_c)
            t_out[v, h, pl.ds(c * f_chunk, f_chunk)] = z.reshape(f_chunk, sub, width).astype(BF16)

            @pl.when(pair < pairs - 1)
            def _():
                lax.fori_loop(0, to_chunk, lambda k, q: (send_chunk(pair, v, h, c * to_chunk + k), q)[1], 0)

            @pl.when(pair == pairs - 1)
            def _():
                pltpu.make_async_copy(t_out.at[v, h, pl.ds(c * f_chunk, f_chunk)], y_ref.at[v, pl.ds(c * f_chunk, f_chunk), h], y_sem.at[v, h]).start()
            return carry

        @pl.when(pair > 0)
        def _():
            part = t_out.at[v, h, pl.ds(0, frames - f_loc)]
            pltpu.make_async_copy(part, part, b_send.at[v, h]).wait()

        lax.fori_loop(0, chunks, phase3, 0)

    def run_pair(pair, carry):
        layer = 2 * pair
        for c in weight_copies(layer):
            c.wait()
        start_weights(layer + 1)
        for v in range(videos):
            @pl.when(pair == 0)
            def _():
                pltpu.make_async_copy(x_ref.at[v], s_in.at[0, v], x_sem.at[v]).wait()

            @pl.when(pair > 0)
            def _():
                pltpu.make_async_copy(x_ref.at[v], s_in.at[1, v], b_recv.at[v]).wait()

            def frame(f, q):
                spatial_frame(pair, v, f)
                if v == 0:
                    @pl.when((f == 0) & (pair == 0))
                    def _():
                        pl.semaphore_wait(barrier, n - 1)
                    send_frame(pair, v, f)
                return q

            lax.fori_loop(0, f_loc, frame, 0)
            if v > 0:
                for h in range(halves):
                    send_half(pair, v, h)
        for c in weight_copies(layer + 1):
            c.wait()

        @pl.when(pair < pairs - 1)
        def _():
            start_weights(layer + 2)

        for v in range(videos):
            if v == 0:
                pltpu.make_async_copy(t_in.at[pair, v], t_in.at[pair, v], ac_recv.at[pair, v, 0]).wait()

            def half(h, q):
                if v > 0:
                    pltpu.make_async_copy(t_in.at[pair, v, h], t_in.at[pair, v, h], ac_recv.at[pair, v, h]).wait()
                temporal(pair, v, h)
                return q

            lax.fori_loop(0, halves, half, 0)
        return carry

    lax.fori_loop(0, pairs, run_pair, 0)

    for v in range(videos):
        for h in range(halves):
            done = y_ref.at[v, :, h]
            pltpu.make_async_copy(done, done, y_sem.at[v, h]).wait()
            for pair in range(pairs):
                part = t_in.at[pair, v, h, pl.ds(0, frames - f_loc)]
                pltpu.make_async_copy(part, part, ac_send.at[pair, v, h if v else 0]).wait()


def solution(mesh):
    n = mesh.shape["sp"]

    def local_stack(x, norms, w_qkv, w_out, w_up, w_down):
        videos, f_loc, patches, width = x.shape
        layers = w_qkv.shape[0]
        pairs = layers // 2
        head = w_qkv.shape[-1]
        hidden = w_up.shape[-1]
        frames, halves = f_loc * n, patches // n // SUB
        x = x.reshape(videos, f_loc, patches // SUB, SUB, width)
        w_qkv = w_qkv.transpose(0, 2, 3, 4, 1).reshape(layers, 3 * width, width)
        w_out = w_out.reshape(layers, width, width)
        any_space = pl.BlockSpec(memory_space=pl.ANY)
        y = pl.pallas_call(
            functools.partial(kernel, n, head),
            out_shape=jax.ShapeDtypeStruct((videos, frames, halves, SUB, width), BF16),
            in_specs=[any_space, pl.BlockSpec(memory_space=pltpu.VMEM)] + [any_space] * 4,
            out_specs=any_space,
            scratch_shapes=[
                pltpu.VMEM((layers, 3 * width, width), BF16),
                pltpu.VMEM((layers, width, width), BF16),
                pltpu.VMEM((layers, width, hidden), BF16),
                pltpu.VMEM((layers, hidden, width), BF16),
                pltpu.VMEM((pairs, videos, f_loc, patches // SUB, SUB, width), BF16),
                pltpu.VMEM((pairs, videos, f_loc, patches // SUB, SUB, width), BF16),
                pltpu.VMEM((pairs, videos, halves, frames, SUB, width), BF16),
                pltpu.VMEM((videos, halves, frames, SUB, width), BF16),
                pltpu.VMEM((width // head, LANES, patches), BF16),
                pltpu.VMEM((patches, width), BF16),
                pltpu.VMEM((width, patches), BF16),
                pltpu.VMEM((patches, width), BF16),
                pltpu.VMEM((width, patches), BF16),
                pltpu.VMEM((width // head, patches, patches), F32),
                pltpu.VMEM((width // head, patches, patches), BF16),
                pltpu.VMEM((patches, hidden), BF16),
                pltpu.VMEM((width // LANES, frames * SUB, LANES), F32),
                pltpu.VMEM((width // LANES, frames * SUB, LANES), F32),
                pltpu.VMEM((4 * frames, 4 * frames), F32),
                pltpu.SemaphoreType.DMA((layers, 4)),
                pltpu.SemaphoreType.DMA((videos,)),
                pltpu.SemaphoreType.DMA((videos,)),
                pltpu.SemaphoreType.DMA((pairs, videos, halves)),
                pltpu.SemaphoreType.DMA((videos, halves)),
                pltpu.SemaphoreType.DMA((pairs, videos, halves)),
                pltpu.SemaphoreType.DMA((videos, halves)),
            ],
            compiler_params=pltpu.CompilerParams(collective_id=0, has_side_effects=True, vmem_limit_bytes=60 * 1024 * 1024),
            name="stack",
        )(x, norms, w_qkv, w_out, w_up, w_down)
        return y.reshape(videos, frames, halves * SUB, width)

    replicated = P()
    return jax.shard_map(local_stack, mesh=mesh, in_specs=(P('data', 'sp', None, None), replicated, replicated, replicated, replicated, replicated), out_specs=P('data', None, 'sp', None), check_vma=False)
```

```python
import functools
import math
import jax
import jax.numpy as jnp
from jax import lax
from jax.experimental import pallas as pl
from jax.experimental.pallas import tpu as pltpu
from jax.sharding import PartitionSpec as P

EPS = 1e-6
LANES = 128
SUB = 8
MASKED = -1e38
GELU_A, GELU_B = math.sqrt(2 / math.pi), 0.044715
F32, BF16 = jnp.float32, jnp.bfloat16


def dot(a, b):
    return jnp.dot(a, b, preferred_element_type=F32)


def dot_nt(a, b):
    return lax.dot_general(a, b, (((1,), (1,)), ((), ())), preferred_element_type=F32)


def dot_tn(a, b):
    return lax.dot_general(a, b, (((0,), (0,)), ((), ())), preferred_element_type=F32)


def layer_norm(x, gain, shift):
    centered = x - jnp.mean(x, axis=-1, keepdims=True)
    variance = jnp.mean(centered * centered, axis=-1, keepdims=True)
    return centered * lax.rsqrt(variance + EPS) * gain + shift


def kernel(n, head, x_ref, norms, wqkv_hbm, wout_hbm, wup_hbm, wdown_hbm, y_ref,
           wqkv, wout, wup, wdown, s_in, s_out, t_in, t_out, q_s, k_s, v_s, ot_s, s_s, hid_s, next_h, next_a, cur_h, cur_a, u_f32, z_f32, mask_s,
           w_sem, x_sem, b_recv, ac_recv, b_send, ac_send, y_sem):
    pairs, videos, f_loc, tiles, sub, width = s_in.shape
    halves, frames = t_in.shape[2], t_in.shape[3]
    patches = tiles * sub
    me = lax.axis_index("sp")
    pair_heads = width // LANES
    group = 4
    rows_g = group * frames
    scale = head ** -0.5

    barrier = pltpu.get_barrier_semaphore()

    def tell(step, c):
        pl.semaphore_signal(barrier, inc=1, device_id={"sp": lax.rem(me + step, n)})
        return c

    lax.fori_loop(1, n, tell, 0)

    def weight_copies(layer):
        return [pltpu.make_async_copy(src.at[layer], dst.at[layer], w_sem.at[layer, i])
                for i, (src, dst) in enumerate(((wqkv_hbm, wqkv), (wout_hbm, wout), (wup_hbm, wup), (wdown_hbm, wdown)))]

    def start_weights(layer):
        for c in weight_copies(layer):
            c.start()

    for v in range(videos):
        pltpu.make_async_copy(x_ref.at[v], s_in.at[0, v], x_sem.at[v]).start()
    start_weights(0)

    row_p = lax.broadcasted_iota(jnp.int32, (rows_g, rows_g), 0)
    col_p = lax.broadcasted_iota(jnp.int32, (rows_g, rows_g), 1)
    same = jnp.zeros((rows_g, rows_g), F32)
    for i in range(group):
        lo, hi = i * frames, (i + 1) * frames
        inside = (row_p >= lo) & (row_p < hi) & (col_p >= lo) & (col_p < hi)
        same = jnp.where(inside, 1.0, same)
    mask_s[...] = same

    q_s[...] = jnp.zeros_like(q_s)

    heads = width // head

    def scores(h, rows, masked):
        s = dot(k_s[pl.ds(0, rows), pl.ds(h * head // LANES * LANES, LANES)], q_s[h, :, pl.ds(0, rows)])
        if masked:
            s = jnp.where(mask_s[...] > 0.5, s, MASKED)
        s_s[h, pl.ds(0, rows), pl.ds(0, rows)] = s
        return jnp.max(s, axis=0, keepdims=True) + math.log(rows)

    def mix(h, rows, top):
        e = jnp.exp(s_s[h, pl.ds(0, rows), pl.ds(0, rows)] - top)
        o = dot(v_s[pl.ds(h * head, head), pl.ds(0, rows)], e.astype(BF16))
        ot_s[pl.ds(h * head, head), pl.ds(0, rows)] = (o * (1.0 / jnp.sum(e, axis=0, keepdims=True))).astype(BF16)

    def gelu(x):
        t = jnp.tanh(x * (GELU_A + (GELU_A * GELU_B) * (x * x)))
        half = 0.5 * x
        return half + half * t

    def attention_steps(get, rows, layer, masked):
        a = layer_norm(get(), norms[layer, pl.ds(0, 1), :], norms[layer, pl.ds(1, 1), :]).astype(BF16)
        yield
        q = (dot_nt(wqkv[layer, pl.ds(0, width), :], a) * scale).astype(BF16)
        for h in range(heads):
            q_s[h, pl.ds(h * head % LANES, head), pl.ds(0, rows)] = q[h * head:(h + 1) * head]
        yield
        k_s[pl.ds(0, rows), :] = dot_nt(a, wqkv[layer, pl.ds(width, width), :]).astype(BF16)
        yield
        v_s[:, pl.ds(0, rows)] = dot_nt(wqkv[layer, pl.ds(2 * width, width), :], a).astype(BF16)
        yield
        ahead = 2
        tops = [scores(h, rows, masked) for h in range(ahead)]
        yield
        for h in range(heads):
            if h + ahead < heads:
                tops.append(scores(h + ahead, rows, masked))
            mix(h, rows, tops[h])
            yield
        h = (get() + dot_tn(ot_s[:, pl.ds(0, rows)], wout[layer])).astype(BF16)
        next_h[pl.ds(0, rows), :] = h
        next_a[pl.ds(0, rows), :] = layer_norm(h.astype(F32), norms[layer, pl.ds(2, 1), :], norms[layer, pl.ds(3, 1), :]).astype(BF16)
        yield

    def mlp_steps(rows, layer, put):
        cur_h[pl.ds(0, rows), :] = next_h[pl.ds(0, rows), :]
        cur_a[pl.ds(0, rows), :] = next_a[pl.ds(0, rows), :]
        chunk = 256
        for c in range(hid_s.shape[1] // chunk):
            up = dot(cur_a[pl.ds(0, rows), :], wup[layer, :, pl.ds(c * chunk, chunk)])
            hid_s[pl.ds(0, rows), pl.ds(c * chunk, chunk)] = gelu(up).astype(BF16)
            yield
        put(cur_h[pl.ds(0, rows), :].astype(F32) + dot(hid_s[pl.ds(0, rows), :], wdown[layer]))
        yield

    def emit(first, second):
        steps = "ABAABAABAABAABAABAB" if first is not None and second is not None else "A" * 12 + "B" * 7
        for step in steps:
            stage = first if step == "A" else second
            if stage is not None:
                next(stage)

    def pipeline(tiles_n, attention, mlp, before, after):
        before(0)
        emit(attention(0), None)

        def step(i, c):
            before(i)
            emit(attention(i), mlp(i - 1))
            after(i - 1)
            return c

        lax.fori_loop(1, tiles_n, step, 0)
        emit(None, mlp(tiles_n - 1))
        after(tiles_n - 1)

    def spread(send):
        def both(i, c):
            send(lax.rem(me + n // 2 + i, n))

            @pl.when(i > 0)
            def _():
                send(lax.rem(me + n // 2 + n - i, n))
            return c

        lax.fori_loop(0, n // 2, both, 0)

    def send_frame(pair, v, f):
        def part(to):
            return s_out.at[pair, v, f, pl.ds(to * halves, halves)], t_in.at[pair, v, :, me * f_loc + f]

        def send(to):
            src, dst = part(to)
            pltpu.make_async_remote_copy(src_ref=src, dst_ref=dst, send_sem=ac_send.at[pair, v, 0], recv_sem=ac_recv.at[pair, v, 0], device_id={"sp": to}).start()

        src, dst = part(me)
        pltpu.make_async_copy(src, dst, ac_recv.at[pair, v, 0]).start()
        spread(send)

    def send_half(pair, v, h):
        def part(to):
            return s_out.at[pair, v, :, to * halves + h], t_in.at[pair, v, h, pl.ds(me * f_loc, f_loc)]

        def send(to):
            src, dst = part(to)
            pltpu.make_async_remote_copy(src_ref=src, dst_ref=dst, send_sem=ac_send.at[pair, v, h], recv_sem=ac_recv.at[pair, v, h], device_id={"sp": to}).start()

        src, dst = part(me)
        pltpu.make_async_copy(src, dst, ac_recv.at[pair, v, h]).start()
        spread(send)

    def spatial(pair):
        layer = 2 * pair

        def before(i):
            @pl.when(lax.rem(i, f_loc) == 0)
            def _():
                v = i // f_loc

                @pl.when(pair == 0)
                def _():
                    pltpu.make_async_copy(x_ref.at[v], s_in.at[0, v], x_sem.at[v]).wait()

                @pl.when(pair > 0)
                def _():
                    pltpu.make_async_copy(x_ref.at[v], s_in.at[1, v], b_recv.at[v]).wait()

        def attention(i):
            return attention_steps(lambda: s_in[pair, i // f_loc, lax.rem(i, f_loc)].astype(F32).reshape(patches, width), patches, layer, False)

        def mlp(i):
            def put(z):
                s_out[pair, i // f_loc, lax.rem(i, f_loc)] = z.reshape(tiles, sub, width).astype(BF16)

            return mlp_steps(patches, layer, put)

        def after(i):
            v, f = i // f_loc, lax.rem(i, f_loc)

            @pl.when((pair == 0) & (i == 0))
            def _():
                pl.semaphore_wait(barrier, n - 1)

            @pl.when(v == 0)
            def _():
                send_frame(pair, v, f)

            @pl.when((v > 0) & (f == f_loc - 1))
            def _():
                for h in range(halves):
                    send_half(pair, v, h)

        pipeline(videos * f_loc, attention, mlp, before, after)

    def temporal(pair):
        layer = 2 * pair + 1
        groups = sub // group
        chunks = 2
        f_chunk = frames // chunks
        rows_c = f_chunk * sub

        def place(i):
            return i // (groups * halves), lax.rem(i // groups, halves), lax.rem(i, groups)

        def before(i):
            v, h, g = place(i)

            @pl.when(g == 0)
            def _():
                @pl.when((v == 0) & (h == 0))
                def _():
                    pltpu.make_async_copy(t_in.at[pair, 0], t_in.at[pair, 0], ac_recv.at[pair, 0, 0]).wait()

                @pl.when(v > 0)
                def _():
                    pltpu.make_async_copy(t_in.at[pair, v, h], t_in.at[pair, v, h], ac_recv.at[pair, v, h]).wait()

                def widen(c, q):
                    u = t_in[pair, v, h, pl.ds(c * f_chunk, f_chunk)].astype(F32).reshape(rows_c, width)
                    for j in range(pair_heads):
                        u_f32[j, pl.ds(pl.multiple_of(c * rows_c, rows_c), rows_c), :] = u[:, j * LANES:(j + 1) * LANES]
                    return q

                lax.fori_loop(0, chunks, widen, 0)

        def attention(i):
            g = place(i)[2]

            def get():
                return jnp.concatenate([jnp.concatenate([u_f32[j, pl.ds(g * group + p, frames, stride=sub), :] for p in range(group)], axis=0)
                                        for j in range(pair_heads)], axis=1)

            return attention_steps(get, rows_g, layer, True)

        def mlp(i):
            g = place(i)[2]

            def put(z):
                for p in range(group):
                    for j in range(pair_heads):
                        z_f32[j, pl.ds(g * group + p, frames, stride=sub), :] = z[p * frames:(p + 1) * frames, j * LANES:(j + 1) * LANES]

            return mlp_steps(rows_g, layer, put)

        def after(i):
            v, h, g = place(i)

            @pl.when(g == groups - 1)
            def _():
                @pl.when(pair > 0)
                def _():
                    part = t_out.at[v, h, pl.ds(0, frames - f_loc)]
                    pltpu.make_async_copy(part, part, b_send.at[v, h]).wait()

                def narrow(c, q):
                    rows = pl.ds(pl.multiple_of(c * rows_c, rows_c), rows_c)
                    z = jnp.concatenate([z_f32[j, rows, :] for j in range(pair_heads)], axis=1)
                    t_out[v, h, pl.ds(c * f_chunk, f_chunk)] = z.reshape(f_chunk, sub, width).astype(BF16)
                    return q

                lax.fori_loop(0, chunks, narrow, 0)

                @pl.when(pair < pairs - 1)
                def _():
                    def part(to):
                        return t_out.at[v, h, pl.ds(to * f_loc, f_loc)], s_in.at[pair + 1, v, :, me * halves + h]

                    def send(to):
                        src, dst = part(to)
                        pltpu.make_async_remote_copy(src_ref=src, dst_ref=dst, send_sem=b_send.at[v, h], recv_sem=b_recv.at[v], device_id={"sp": to}).start()

                    src, dst = part(me)
                    pltpu.make_async_copy(src, dst, b_recv.at[v]).start()
                    spread(send)

                @pl.when(pair == pairs - 1)
                def _():
                    pltpu.make_async_copy(t_out.at[v, h], y_ref.at[v, :, h], y_sem.at[v, h]).start()

        pipeline(videos * halves * groups, attention, mlp, before, after)

    def run_pair(pair, carry):
        layer = 2 * pair
        for c in weight_copies(layer):
            c.wait()
        start_weights(layer + 1)
        spatial(pair)
        for c in weight_copies(layer + 1):
            c.wait()

        @pl.when(pair < pairs - 1)
        def _():
            start_weights(layer + 2)

        temporal(pair)
        return carry

    lax.fori_loop(0, pairs, run_pair, 0)

    for v in range(videos):
        for h in range(halves):
            done = y_ref.at[v, :, h]
            pltpu.make_async_copy(done, done, y_sem.at[v, h]).wait()
            for pair in range(pairs):
                part = t_in.at[pair, v, h, pl.ds(0, frames - f_loc)]
                pltpu.make_async_copy(part, part, ac_send.at[pair, v, h if v else 0]).wait()


def solution(mesh):
    n = mesh.shape["sp"]

    def local_stack(x, norms, w_qkv, w_out, w_up, w_down):
        videos, f_loc, patches, width = x.shape
        layers = w_qkv.shape[0]
        pairs = layers // 2
        head = w_qkv.shape[-1]
        hidden = w_up.shape[-1]
        frames, halves = f_loc * n, patches // n // SUB
        x = x.reshape(videos, f_loc, patches // SUB, SUB, width)
        w_qkv = w_qkv.transpose(0, 2, 3, 4, 1).reshape(layers, 3 * width, width)
        w_out = w_out.reshape(layers, width, width)
        any_space = pl.BlockSpec(memory_space=pl.ANY)
        y = pl.pallas_call(
            functools.partial(kernel, n, head),
            out_shape=jax.ShapeDtypeStruct((videos, frames, halves, SUB, width), BF16),
            in_specs=[any_space, pl.BlockSpec(memory_space=pltpu.VMEM)] + [any_space] * 4,
            out_specs=any_space,
            scratch_shapes=[
                pltpu.VMEM((layers, 3 * width, width), BF16),
                pltpu.VMEM((layers, width, width), BF16),
                pltpu.VMEM((layers, width, hidden), BF16),
                pltpu.VMEM((layers, hidden, width), BF16),
                pltpu.VMEM((pairs, videos, f_loc, patches // SUB, SUB, width), BF16),
                pltpu.VMEM((pairs, videos, f_loc, patches // SUB, SUB, width), BF16),
                pltpu.VMEM((pairs, videos, halves, frames, SUB, width), BF16),
                pltpu.VMEM((videos, halves, frames, SUB, width), BF16),
                pltpu.VMEM((width // head, LANES, patches), BF16),
                pltpu.VMEM((patches, width), BF16),
                pltpu.VMEM((width, patches), BF16),
                pltpu.VMEM((width, patches), BF16),
                pltpu.VMEM((width // head, patches, patches), F32),
                pltpu.VMEM((patches, hidden), BF16),
                pltpu.VMEM((patches, width), BF16),
                pltpu.VMEM((patches, width), BF16),
                pltpu.VMEM((patches, width), BF16),
                pltpu.VMEM((patches, width), BF16),
                pltpu.VMEM((width // LANES, frames * SUB, LANES), F32),
                pltpu.VMEM((width // LANES, frames * SUB, LANES), F32),
                pltpu.VMEM((4 * frames, 4 * frames), F32),
                pltpu.SemaphoreType.DMA((layers, 4)),
                pltpu.SemaphoreType.DMA((videos,)),
                pltpu.SemaphoreType.DMA((videos,)),
                pltpu.SemaphoreType.DMA((pairs, videos, halves)),
                pltpu.SemaphoreType.DMA((videos, halves)),
                pltpu.SemaphoreType.DMA((pairs, videos, halves)),
                pltpu.SemaphoreType.DMA((videos, halves)),
            ],
            compiler_params=pltpu.CompilerParams(collective_id=0, has_side_effects=True, vmem_limit_bytes=60 * 1024 * 1024),
            name="stack",
        )(x, norms, w_qkv, w_out, w_up, w_down)
        return y.reshape(videos, frames, halves * SUB, width)

    replicated = P()
    return jax.shard_map(local_stack, mesh=mesh, in_specs=(P('data', 'sp', None, None), replicated, replicated, replicated, replicated, replicated), out_specs=P('data', None, 'sp', None), check_vma=False)
```

```python
import functools
import math
import jax
import jax.numpy as jnp
from jax import lax
from jax.experimental import pallas as pl
from jax.experimental.pallas import tpu as pltpu
from jax.sharding import PartitionSpec as P

EPS = 1e-6
LANES = 128
SUB = 8
VMEM_BYTES = 65_700_000
GELU_A, GELU_B = math.sqrt(2 / math.pi), 0.044715
F32, BF16 = jnp.float32, jnp.bfloat16


def dot(a, b):
    return jnp.dot(a, b, preferred_element_type=F32)


def dot_nt(a, b):
    return lax.dot_general(a, b, (((1,), (1,)), ((), ())), preferred_element_type=F32)


def dot_tn(a, b):
    return lax.dot_general(a, b, (((0,), (0,)), ((), ())), preferred_element_type=F32)


def layer_norm(x, gain, shift):
    centered = x - jnp.mean(x, axis=-1, keepdims=True)
    variance = jnp.mean(centered * centered, axis=-1, keepdims=True)
    return centered * lax.rsqrt(variance + EPS) * gain + shift


def kernel(n, head, x_ref, norms, wqkv_hbm, wout_hbm, wup_hbm, wdown_hbm, y_ref,
           wqkv, wout, wup, wdown, s_in, s_out, t_in, t_out, q_s, k_s, v_s, ot_s, s_s, hid_s, next_h, next_a, cur_h, cur_a, u_f32, z_f32, mask_s,
           w_sem, x_sem, b_recv, ac_recv, b_send, ac_send, y_sem):
    pairs, videos, f_loc, tiles, sub, width = s_in.shape
    halves, frames = t_in.shape[2], t_in.shape[3]
    patches = tiles * sub
    me = lax.axis_index("sp")
    pair_heads = width // LANES
    group = 4
    rows_g = group * frames
    scale = head ** -0.5

    barrier = pltpu.get_barrier_semaphore()

    def tell(step, c):
        pl.semaphore_signal(barrier, inc=1, device_id={"sp": lax.rem(me + step, n)})
        return c

    lax.fori_loop(1, n, tell, 0)

    def weight_copies(layer):
        return [pltpu.make_async_copy(src.at[layer], dst.at[layer], w_sem.at[layer, i])
                for i, (src, dst) in enumerate(((wqkv_hbm, wqkv), (wout_hbm, wout), (wup_hbm, wup), (wdown_hbm, wdown)))]

    def start_weights(layer):
        for c in weight_copies(layer):
            c.start()

    for v in range(videos):
        pltpu.make_async_copy(x_ref.at[v], s_in.at[0, v], x_sem.at[v]).start()
    start_weights(0)

    row_p = lax.broadcasted_iota(jnp.int32, (rows_g, rows_g), 0)
    col_p = lax.broadcasted_iota(jnp.int32, (rows_g, rows_g), 1)
    across = jnp.full((rows_g, rows_g), -jnp.inf, F32)
    for i in range(group):
        lo, hi = i * frames, (i + 1) * frames
        inside = (row_p >= lo) & (row_p < hi) & (col_p >= lo) & (col_p < hi)
        across = jnp.where(inside, 0.0, across)
    mask_s[...] = across
    q_s[...] = jnp.zeros_like(q_s)

    heads = width // head

    def strips(rows, masked):
        out = []
        for lo in range(0, rows, LANES):
            hi = min(rows, lo + LANES)
            out.append((lo, hi, lo // frames * frames, -(-hi // frames) * frames) if masked else (lo, hi, 0, rows))
        return out if masked else [(0, rows, 0, rows)]

    def scores(h, rows, masked):
        s = dot(k_s[pl.ds(0, rows), pl.ds(h * head // LANES * LANES, LANES)], q_s[h, :, pl.ds(0, rows)])
        tops = []
        for lo, hi, k0, k1 in strips(rows, masked):
            part = s[k0:k1, lo:hi]
            if masked:
                part = part + mask_s[pl.ds(k0, k1 - k0), pl.ds(lo, hi - lo)]
            s_s[h, pl.ds(k0, k1 - k0), pl.ds(lo, hi - lo)] = part
            tops.append(jnp.max(part, axis=0, keepdims=True) + math.log(rows))
        return tops

    def mix(h, rows, masked, tops):
        cols, sums = [], []
        for (lo, hi, k0, k1), top in zip(strips(rows, masked), tops):
            e = jnp.exp(s_s[h, pl.ds(k0, k1 - k0), pl.ds(lo, hi - lo)] - top)
            sums.append(jnp.sum(e, axis=0, keepdims=True))
            col = [jnp.zeros((k, hi - lo), BF16) for k in (k0,)] if k0 else []
            col.append(e.astype(BF16))
            if k1 < rows:
                col.append(jnp.zeros((rows - k1, hi - lo), BF16))
            cols.append(jnp.concatenate(col, axis=0) if len(col) > 1 else col[0])
        p = jnp.concatenate(cols, axis=1) if len(cols) > 1 else cols[0]
        norm = jnp.concatenate(sums, axis=1) if len(sums) > 1 else sums[0]
        o = dot(v_s[pl.ds(h * head, head), pl.ds(0, rows)], p)
        ot_s[pl.ds(h * head, head), pl.ds(0, rows)] = (o * (1.0 / norm)).astype(BF16)

    def gelu(x):
        t = jnp.tanh(x * (GELU_A + (GELU_A * GELU_B) * (x * x)))
        half = 0.5 * x
        return half + half * t

    def attention_steps(get, rows, layer, masked):
        a = layer_norm(get(), norms[layer, pl.ds(0, 1), :], norms[layer, pl.ds(1, 1), :]).astype(BF16)
        yield
        q = (dot_nt(wqkv[layer, pl.ds(0, width), :], a) * scale).astype(BF16)
        for h in range(heads):
            q_s[h, pl.ds(h * head % LANES, head), pl.ds(0, rows)] = q[h * head:(h + 1) * head]
        yield
        k_s[pl.ds(0, rows), :] = dot_nt(a, wqkv[layer, pl.ds(width, width), :]).astype(BF16)
        yield
        v_s[:, pl.ds(0, rows)] = dot_nt(wqkv[layer, pl.ds(2 * width, width), :], a).astype(BF16)
        yield
        ahead = 2
        tops = [scores(h, rows, masked) for h in range(ahead)]
        yield
        for h in range(heads):
            if h + ahead < heads:
                tops.append(scores(h + ahead, rows, masked))
            mix(h, rows, masked, tops[h])
            yield
        h = (get() + dot_tn(ot_s[:, pl.ds(0, rows)], wout[layer])).astype(BF16)
        next_h[pl.ds(0, rows), :] = h
        next_a[pl.ds(0, rows), :] = layer_norm(h.astype(F32), norms[layer, pl.ds(2, 1), :], norms[layer, pl.ds(3, 1), :]).astype(BF16)
        yield

    def mlp_steps(rows, layer, put):
        cur_h[pl.ds(0, rows), :] = next_h[pl.ds(0, rows), :]
        cur_a[pl.ds(0, rows), :] = next_a[pl.ds(0, rows), :]
        chunk = 256
        for c in range(hid_s.shape[1] // chunk):
            up = dot(cur_a[pl.ds(0, rows), :], wup[layer, :, pl.ds(c * chunk, chunk)])
            hid_s[pl.ds(0, rows), pl.ds(c * chunk, chunk)] = gelu(up).astype(BF16)
            yield
        put(cur_h[pl.ds(0, rows), :].astype(F32) + dot(hid_s[pl.ds(0, rows), :], wdown[layer]))
        yield

    def emit(first, second):
        steps = "ABAABAABAABAABAABAB" if first is not None and second is not None else "A" * 12 + "B" * 7
        for step in steps:
            stage = first if step == "A" else second
            if stage is not None:
                next(stage)

    def pipeline(tiles_n, attention, mlp, before, after):
        before(0)
        emit(attention(0), None)

        def step(i, c):
            before(i)
            emit(attention(i), mlp(i - 1))
            after(i - 1)
            return c

        lax.fori_loop(1, tiles_n, step, 0)
        emit(None, mlp(tiles_n - 1))
        after(tiles_n - 1)

    def spread(send):
        def both(i, c):
            send(lax.rem(me + n // 2 + i, n))

            @pl.when(i > 0)
            def _():
                send(lax.rem(me + n // 2 + n - i, n))
            return c

        lax.fori_loop(0, n // 2, both, 0)

    def send_frame(pair, v, f):
        def part(to):
            return s_out.at[pair, v, f, pl.ds(to * halves, halves)], t_in.at[pair, v, :, me * f_loc + f]

        def send(to):
            src, dst = part(to)
            pltpu.make_async_remote_copy(src_ref=src, dst_ref=dst, send_sem=ac_send.at[pair, v, 0], recv_sem=ac_recv.at[pair, v, 0], device_id={"sp": to}).start()

        src, dst = part(me)
        pltpu.make_async_copy(src, dst, ac_recv.at[pair, v, 0]).start()
        spread(send)

    def send_half(pair, v, h):
        def part(to):
            return s_out.at[pair, v, :, to * halves + h], t_in.at[pair, v, h, pl.ds(me * f_loc, f_loc)]

        def send(to):
            src, dst = part(to)
            pltpu.make_async_remote_copy(src_ref=src, dst_ref=dst, send_sem=ac_send.at[pair, v, h], recv_sem=ac_recv.at[pair, v, h], device_id={"sp": to}).start()

        src, dst = part(me)
        pltpu.make_async_copy(src, dst, ac_recv.at[pair, v, h]).start()
        spread(send)

    def spatial(pair):
        layer = 2 * pair

        def before(i):
            @pl.when(lax.rem(i, f_loc) == 0)
            def _():
                v = i // f_loc

                @pl.when(pair == 0)
                def _():
                    pltpu.make_async_copy(x_ref.at[v], s_in.at[0, v], x_sem.at[v]).wait()

                @pl.when(pair > 0)
                def _():
                    pltpu.make_async_copy(x_ref.at[v], s_in.at[1, v], b_recv.at[v]).wait()

        def attention(i):
            return attention_steps(lambda: s_in[pair, i // f_loc, lax.rem(i, f_loc)].astype(F32).reshape(patches, width), patches, layer, False)

        def mlp(i):
            def put(z):
                s_out[pair, i // f_loc, lax.rem(i, f_loc)] = z.reshape(tiles, sub, width).astype(BF16)

            return mlp_steps(patches, layer, put)

        def after(i):
            v, f = i // f_loc, lax.rem(i, f_loc)

            @pl.when((pair == 0) & (i == 0))
            def _():
                pl.semaphore_wait(barrier, n - 1)

            @pl.when(v == 0)
            def _():
                send_frame(pair, v, f)

            @pl.when((v > 0) & (f == f_loc - 1))
            def _():
                for h in range(halves):
                    send_half(pair, v, h)

        pipeline(videos * f_loc, attention, mlp, before, after)

    def temporal(pair):
        layer = 2 * pair + 1
        groups = sub // group
        chunks = 2
        f_chunk = frames // chunks
        rows_c = f_chunk * sub

        def place(i):
            return i // (groups * halves), lax.rem(i // groups, halves), lax.rem(i, groups)

        def before(i):
            v, h, g = place(i)

            @pl.when(g == 0)
            def _():
                @pl.when((v == 0) & (h == 0))
                def _():
                    pltpu.make_async_copy(t_in.at[pair, 0], t_in.at[pair, 0], ac_recv.at[pair, 0, 0]).wait()

                @pl.when(v > 0)
                def _():
                    pltpu.make_async_copy(t_in.at[pair, v, h], t_in.at[pair, v, h], ac_recv.at[pair, v, h]).wait()

                def widen(c, q):
                    u = t_in[pair, v, h, pl.ds(c * f_chunk, f_chunk)].astype(F32).reshape(rows_c, width)
                    for j in range(pair_heads):
                        u_f32[j, pl.ds(pl.multiple_of(c * rows_c, rows_c), rows_c), :] = u[:, j * LANES:(j + 1) * LANES]
                    return q

                lax.fori_loop(0, chunks, widen, 0)

        def attention(i):
            g = place(i)[2]

            def get():
                return jnp.concatenate([jnp.concatenate([u_f32[j, pl.ds(g * group + p, frames, stride=sub), :] for p in range(group)], axis=0)
                                        for j in range(pair_heads)], axis=1)

            return attention_steps(get, rows_g, layer, True)

        def mlp(i):
            g = place(i)[2]

            def put(z):
                for p in range(group):
                    for j in range(pair_heads):
                        z_f32[j, pl.ds(g * group + p, frames, stride=sub), :] = z[p * frames:(p + 1) * frames, j * LANES:(j + 1) * LANES]

            return mlp_steps(rows_g, layer, put)

        def after(i):
            v, h, g = place(i)

            @pl.when(g == groups - 1)
            def _():
                @pl.when(pair > 0)
                def _():
                    part = t_out.at[v, h, pl.ds(0, frames - f_loc)]
                    pltpu.make_async_copy(part, part, b_send.at[v, h]).wait()

                def narrow(c, q):
                    rows = pl.ds(pl.multiple_of(c * rows_c, rows_c), rows_c)
                    z = jnp.concatenate([z_f32[j, rows, :] for j in range(pair_heads)], axis=1)
                    t_out[v, h, pl.ds(c * f_chunk, f_chunk)] = z.reshape(f_chunk, sub, width).astype(BF16)
                    return q

                lax.fori_loop(0, chunks, narrow, 0)

                @pl.when(pair < pairs - 1)
                def _():
                    def part(to):
                        return t_out.at[v, h, pl.ds(to * f_loc, f_loc)], s_in.at[pair + 1, v, :, me * halves + h]

                    def send(to):
                        src, dst = part(to)
                        pltpu.make_async_remote_copy(src_ref=src, dst_ref=dst, send_sem=b_send.at[v, h], recv_sem=b_recv.at[v], device_id={"sp": to}).start()

                    src, dst = part(me)
                    pltpu.make_async_copy(src, dst, b_recv.at[v]).start()
                    spread(send)

                @pl.when(pair == pairs - 1)
                def _():
                    pltpu.make_async_copy(t_out.at[v, h], y_ref.at[v, :, h], y_sem.at[v, h]).start()

        pipeline(videos * halves * groups, attention, mlp, before, after)

    def run_pair(pair, carry):
        layer = 2 * pair
        for c in weight_copies(layer):
            c.wait()
        start_weights(layer + 1)
        spatial(pair)
        for c in weight_copies(layer + 1):
            c.wait()

        @pl.when(pair < pairs - 1)
        def _():
            start_weights(layer + 2)

        temporal(pair)
        return carry

    lax.fori_loop(0, pairs, run_pair, 0)

    for v in range(videos):
        for h in range(halves):
            done = y_ref.at[v, :, h]
            pltpu.make_async_copy(done, done, y_sem.at[v, h]).wait()
            for pair in range(pairs):
                part = t_in.at[pair, v, h, pl.ds(0, frames - f_loc)]
                pltpu.make_async_copy(part, part, ac_send.at[pair, v, h if v else 0]).wait()


def solution(mesh):
    n = mesh.shape["sp"]

    def local_stack(x, norms, w_qkv, w_out, w_up, w_down):
        videos, f_loc, patches, width = x.shape
        layers = w_qkv.shape[0]
        pairs = layers // 2
        head = w_qkv.shape[-1]
        hidden = w_up.shape[-1]
        frames, halves = f_loc * n, patches // n // SUB
        x = x.reshape(videos, f_loc, patches // SUB, SUB, width)
        w_qkv = w_qkv.transpose(0, 2, 3, 4, 1).reshape(layers, 3 * width, width)
        w_out = w_out.reshape(layers, width, width)
        any_space = pl.BlockSpec(memory_space=pl.ANY)
        y = pl.pallas_call(
            functools.partial(kernel, n, head),
            out_shape=pltpu.VMEM((videos, frames, halves, SUB, width), BF16),
            in_specs=[any_space, pl.BlockSpec(memory_space=pltpu.VMEM)] + [any_space] * 4,
            out_specs=pl.BlockSpec(memory_space=pltpu.VMEM),
            scratch_shapes=[
                pltpu.VMEM((layers, 3 * width, width), BF16),
                pltpu.VMEM((layers, width, width), BF16),
                pltpu.VMEM((layers, width, hidden), BF16),
                pltpu.VMEM((layers, hidden, width), BF16),
                pltpu.VMEM((pairs, videos, f_loc, patches // SUB, SUB, width), BF16),
                pltpu.VMEM((pairs, videos, f_loc, patches // SUB, SUB, width), BF16),
                pltpu.VMEM((pairs, videos, halves, frames, SUB, width), BF16),
                pltpu.VMEM((videos, halves, frames, SUB, width), BF16),
                pltpu.VMEM((width // head, LANES, patches), BF16),
                pltpu.VMEM((patches, width), BF16),
                pltpu.VMEM((width, patches), BF16),
                pltpu.VMEM((width, patches), BF16),
                pltpu.VMEM((width // head, patches, patches), F32),
                pltpu.VMEM((patches, hidden), BF16),
                pltpu.VMEM((patches, width), BF16),
                pltpu.VMEM((patches, width), BF16),
                pltpu.VMEM((patches, width), BF16),
                pltpu.VMEM((patches, width), BF16),
                pltpu.VMEM((width // LANES, frames * SUB, LANES), F32),
                pltpu.VMEM((width // LANES, frames * SUB, LANES), F32),
                pltpu.VMEM((4 * frames, 4 * frames), F32),
                pltpu.SemaphoreType.DMA((layers, 4)),
                pltpu.SemaphoreType.DMA((videos,)),
                pltpu.SemaphoreType.DMA((videos,)),
                pltpu.SemaphoreType.DMA((pairs, videos, halves)),
                pltpu.SemaphoreType.DMA((videos, halves)),
                pltpu.SemaphoreType.DMA((pairs, videos, halves)),
                pltpu.SemaphoreType.DMA((videos, halves)),
            ],
            compiler_params=pltpu.CompilerParams(collective_id=0, has_side_effects=True, vmem_limit_bytes=VMEM_BYTES),
            name="stack",
        )(x, norms, w_qkv, w_out, w_up, w_down)
        return y.reshape(videos, frames, halves * SUB, width)

    replicated = P()
    return jax.shard_map(local_stack, mesh=mesh, in_specs=(P('data', 'sp', None, None), replicated, replicated, replicated, replicated, replicated), out_specs=P('data', None, 'sp', None), check_vma=False)
```

```python
import functools
import math
import jax
import jax.numpy as jnp
from jax import lax
from jax.experimental import pallas as pl
from jax.experimental.pallas import tpu as pltpu
from jax.sharding import PartitionSpec as P

EPS = 1e-6
LANES = 128
SUB = 8
VMEM_BYTES = 65_700_000
ATTENTION_STEPS, MLP_STEPS = 12, 7
GELU_A, GELU_B = math.sqrt(2 / math.pi), 0.044715
F32, BF16 = jnp.float32, jnp.bfloat16


def dot(a, b):
    return jnp.dot(a, b, preferred_element_type=F32)


def dot_nt(a, b):
    return lax.dot_general(a, b, (((1,), (1,)), ((), ())), preferred_element_type=F32)


def dot_tn(a, b):
    return lax.dot_general(a, b, (((0,), (0,)), ((), ())), preferred_element_type=F32)


def layer_norm(x, gain, shift):
    centered = x - jnp.mean(x, axis=-1, keepdims=True)
    variance = jnp.mean(centered * centered, axis=-1, keepdims=True)
    return centered * lax.rsqrt(variance + EPS) * gain + shift


def kernel(n, head, x_ref, norms, wqkv_hbm, wout_hbm, wup_hbm, wdown_hbm, y_ref,
           wqkv, wout, wup, wdown, s_in, s_out, t_in, t_out, q_s, k_s, v_s, ot_s, s_s, hid_s, next_h, next_a, cur_h, cur_a, u_f32, z_f32, mask_s,
           w_sem, x_sem, b_recv, ac_recv, b_send, ac_send, y_sem):
    pairs, videos, f_loc, tiles, sub, width = s_in.shape
    halves, frames = t_in.shape[2], t_in.shape[3]
    patches = tiles * sub
    me = lax.axis_index("sp")
    pair_heads = width // LANES
    group = 4
    rows_g = group * frames
    scale = head ** -0.5

    barrier = pltpu.get_barrier_semaphore()

    def tell(step, c):
        pl.semaphore_signal(barrier, inc=1, device_id={"sp": lax.rem(me + step, n)})
        return c

    lax.fori_loop(1, n, tell, 0)

    weights = ((wqkv_hbm, wqkv), (wout_hbm, wout), (wup_hbm, wup), (wdown_hbm, wdown))

    def weight_copy(layer, i):
        src, dst = weights[i]
        return pltpu.make_async_copy(src.at[layer], dst.at[layer], w_sem.at[layer, i])

    def start_weights(layer):
        for i in range(len(weights)):
            weight_copy(layer, i).start()

    def wait_weights(layer, which):
        for i in which:
            weight_copy(layer, i).wait()

    for v in range(videos):
        pltpu.make_async_copy(x_ref.at[v], s_in.at[0, v], x_sem.at[v]).start()
    start_weights(0)

    row_p = lax.broadcasted_iota(jnp.int32, (rows_g, rows_g), 0)
    col_p = lax.broadcasted_iota(jnp.int32, (rows_g, rows_g), 1)
    across = jnp.full((rows_g, rows_g), -jnp.inf, F32)
    for i in range(group):
        lo, hi = i * frames, (i + 1) * frames
        inside = (row_p >= lo) & (row_p < hi) & (col_p >= lo) & (col_p < hi)
        across = jnp.where(inside, 0.0, across)
    mask_s[...] = across
    q_s[...] = jnp.zeros_like(q_s)

    heads = width // head

    def strips(rows, masked):
        out = []
        for lo in range(0, rows, LANES):
            hi = min(rows, lo + LANES)
            out.append((lo, hi, lo // frames * frames, -(-hi // frames) * frames) if masked else (lo, hi, 0, rows))
        return out if masked else [(0, rows, 0, rows)]

    def scores(h, rows, masked):
        s = dot(k_s[pl.ds(0, rows), pl.ds(h * head // LANES * LANES, LANES)], q_s[h, :, pl.ds(0, rows)])
        tops = []
        for lo, hi, k0, k1 in strips(rows, masked):
            part = s[k0:k1, lo:hi]
            if masked:
                part = part + mask_s[pl.ds(k0, k1 - k0), pl.ds(lo, hi - lo)]
            s_s[h, pl.ds(k0, k1 - k0), pl.ds(lo, hi - lo)] = part
            tops.append(jnp.max(part, axis=0, keepdims=True) + math.log(rows))
        return tops

    def mix(h, rows, masked, tops):
        cols, sums = [], []
        for (lo, hi, k0, k1), top in zip(strips(rows, masked), tops):
            e = jnp.exp(s_s[h, pl.ds(k0, k1 - k0), pl.ds(lo, hi - lo)] - top)
            sums.append(jnp.sum(e, axis=0, keepdims=True))
            col = [jnp.zeros((k, hi - lo), BF16) for k in (k0,)] if k0 else []
            col.append(e.astype(BF16))
            if k1 < rows:
                col.append(jnp.zeros((rows - k1, hi - lo), BF16))
            cols.append(jnp.concatenate(col, axis=0) if len(col) > 1 else col[0])
        p = jnp.concatenate(cols, axis=1) if len(cols) > 1 else cols[0]
        norm = jnp.concatenate(sums, axis=1) if len(sums) > 1 else sums[0]
        o = dot(v_s[pl.ds(h * head, head), pl.ds(0, rows)], p)
        ot_s[pl.ds(h * head, head), pl.ds(0, rows)] = (o * (1.0 / norm)).astype(BF16)

    def gelu(x):
        t = jnp.tanh(x * (GELU_A + (GELU_A * GELU_B) * (x * x)))
        half = 0.5 * x
        return half + half * t

    def attention_steps(get, rows, layer, masked):
        a = layer_norm(get(), norms[layer, pl.ds(0, 1), :], norms[layer, pl.ds(1, 1), :]).astype(BF16)
        yield
        q = (dot_nt(wqkv[layer, pl.ds(0, width), :], a) * scale).astype(BF16)
        for h in range(heads):
            q_s[h, pl.ds(h * head % LANES, head), pl.ds(0, rows)] = q[h * head:(h + 1) * head]
        yield
        k_s[pl.ds(0, rows), :] = dot_nt(a, wqkv[layer, pl.ds(width, width), :]).astype(BF16)
        yield
        v_s[:, pl.ds(0, rows)] = dot_nt(wqkv[layer, pl.ds(2 * width, width), :], a).astype(BF16)
        yield
        ahead = 2
        tops = [scores(h, rows, masked) for h in range(ahead)]
        yield
        for h in range(heads):
            if h + ahead < heads:
                tops.append(scores(h + ahead, rows, masked))
            mix(h, rows, masked, tops[h])
            yield
        h = (get() + dot_tn(ot_s[:, pl.ds(0, rows)], wout[layer])).astype(BF16)
        next_h[pl.ds(0, rows), :] = h
        next_a[pl.ds(0, rows), :] = layer_norm(h.astype(F32), norms[layer, pl.ds(2, 1), :], norms[layer, pl.ds(3, 1), :]).astype(BF16)
        yield

    def mlp_steps(rows, layer, put):
        cur_h[pl.ds(0, rows), :] = next_h[pl.ds(0, rows), :]
        cur_a[pl.ds(0, rows), :] = next_a[pl.ds(0, rows), :]
        chunk = 256
        for c in range(hid_s.shape[1] // chunk):
            up = dot(cur_a[pl.ds(0, rows), :], wup[layer, :, pl.ds(c * chunk, chunk)])
            hid_s[pl.ds(0, rows), pl.ds(c * chunk, chunk)] = gelu(up).astype(BF16)
            yield
        put(cur_h[pl.ds(0, rows), :].astype(F32) + dot(hid_s[pl.ds(0, rows), :], wdown[layer]))
        yield

    def emit(first, second):
        steps = "ABAABAABAABAABAABAB" if first is not None and second is not None else "A" * ATTENTION_STEPS + "B" * MLP_STEPS
        for step in steps:
            stage = first if step == "A" else second
            if stage is not None:
                next(stage)

    def pipeline(tiles_n, attention, mlp, after, alone=None, late=None):
        steps = attention(0)
        for _ in range(ATTENTION_STEPS - 1):
            next(steps)
        if late is not None:
            late()
        next(steps)
        start = 1
        if alone is not None:
            @pl.when(alone)
            def _():
                emit(None, mlp(0))
                after(0)
                emit(attention(1), None)

            start = jnp.where(alone, 2, 1)

        def step(i, c):
            emit(attention(i), mlp(i - 1))
            after(i - 1)
            return c

        lax.fori_loop(start, tiles_n, step, 0)
        emit(None, mlp(tiles_n - 1))
        after(tiles_n - 1)

    def spread(send):
        def both(i, c):
            send(lax.rem(me + n // 2 + i, n))

            @pl.when(i > 0)
            def _():
                send(lax.rem(me + n // 2 + n - i, n))
            return c

        lax.fori_loop(0, n // 2, both, 0)

    def send_frame(pair, v, f):
        def part(to):
            return s_out.at[pair, v, f, pl.ds(to * halves, halves)], t_in.at[pair, v, :, me * f_loc + f]

        def send(to):
            src, dst = part(to)
            pltpu.make_async_remote_copy(src_ref=src, dst_ref=dst, send_sem=ac_send.at[pair, v, 0], recv_sem=ac_recv.at[pair, v, 0], device_id={"sp": to}).start()

        src, dst = part(me)
        pltpu.make_async_copy(src, dst, ac_recv.at[pair, v, 0]).start()
        spread(send)

    def send_half(pair, v, h):
        def part(to):
            return s_out.at[pair, v, :, to * halves + h], t_in.at[pair, v, h, pl.ds(me * f_loc, f_loc)]

        def send(to):
            src, dst = part(to)
            pltpu.make_async_remote_copy(src_ref=src, dst_ref=dst, send_sem=ac_send.at[pair, v, h], recv_sem=ac_recv.at[pair, v, h], device_id={"sp": to}).start()

        src, dst = part(me)
        pltpu.make_async_copy(src, dst, ac_recv.at[pair, v, h]).start()
        spread(send)

    def spatial(pair):
        layer = 2 * pair

        def video(v, c):
            @pl.when(pair == 0)
            def _():
                pltpu.make_async_copy(x_ref.at[v], s_in.at[0, v], x_sem.at[v]).wait()

            @pl.when(pair > 0)
            def _():
                pltpu.make_async_copy(x_ref.at[v], s_in.at[1, v], b_recv.at[v]).wait()

            def attention(f):
                return attention_steps(lambda: s_in[pair, v, f].astype(F32).reshape(patches, width), patches, layer, False)

            def mlp(f):
                def put(z):
                    s_out[pair, v, f] = z.reshape(tiles, sub, width).astype(BF16)

                return mlp_steps(patches, layer, put)

            def after(f):
                @pl.when((pair == 0) & (v == 0) & (f == 0))
                def _():
                    pl.semaphore_wait(barrier, n - 1)

                @pl.when(v == 0)
                def _():
                    send_frame(pair, v, f)

                @pl.when((v > 0) & (f == f_loc - 1))
                def _():
                    for h in range(halves):
                        send_half(pair, v, h)

            def late():
                @pl.when(v == 0)
                def _():
                    wait_weights(layer, (1, 2, 3))
                    start_weights(layer + 1)

            pipeline(f_loc, attention, mlp, after, (pair == 0) & (v == 0), late)
            return c

        lax.fori_loop(0, videos, video, 0)

    def temporal(pair):
        layer = 2 * pair + 1
        groups = sub // group
        chunks = 2
        f_chunk = frames // chunks
        rows_c = f_chunk * sub

        def unit(i, carry):
            v, h = i // halves, lax.rem(i, halves)

            @pl.when((v == 0) & (h == 0))
            def _():
                pltpu.make_async_copy(t_in.at[pair, 0], t_in.at[pair, 0], ac_recv.at[pair, 0, 0]).wait()

            @pl.when(v > 0)
            def _():
                pltpu.make_async_copy(t_in.at[pair, v, h], t_in.at[pair, v, h], ac_recv.at[pair, v, h]).wait()

            def widen(c, q):
                u = t_in[pair, v, h, pl.ds(c * f_chunk, f_chunk)].astype(F32).reshape(rows_c, width)
                for j in range(pair_heads):
                    u_f32[j, pl.ds(pl.multiple_of(c * rows_c, rows_c), rows_c), :] = u[:, j * LANES:(j + 1) * LANES]
                return q

            lax.fori_loop(0, chunks, widen, 0)
            pipeline(groups, attention, mlp, lambda g: None)
            finish(v, h)
            return carry

        def attention(g):
            def get():
                return jnp.concatenate([jnp.concatenate([u_f32[j, pl.ds(g * group + p, frames, stride=sub), :] for p in range(group)], axis=0)
                                        for j in range(pair_heads)], axis=1)

            return attention_steps(get, rows_g, layer, True)

        def mlp(g):
            def put(z):
                for p in range(group):
                    for j in range(pair_heads):
                        z_f32[j, pl.ds(g * group + p, frames, stride=sub), :] = z[p * frames:(p + 1) * frames, j * LANES:(j + 1) * LANES]

            return mlp_steps(rows_g, layer, put)

        def finish(v, h):
            @pl.when(pair > 0)
            def _():
                part = t_out.at[v, h, pl.ds(0, frames - f_loc)]
                pltpu.make_async_copy(part, part, b_send.at[v, h]).wait()

            def narrow(c, q):
                rows = pl.ds(pl.multiple_of(c * rows_c, rows_c), rows_c)
                z = jnp.concatenate([z_f32[j, rows, :] for j in range(pair_heads)], axis=1)
                t_out[v, h, pl.ds(c * f_chunk, f_chunk)] = z.reshape(f_chunk, sub, width).astype(BF16)
                return q

            lax.fori_loop(0, chunks, narrow, 0)

            @pl.when(pair < pairs - 1)
            def _():
                def part(to):
                    return t_out.at[v, h, pl.ds(to * f_loc, f_loc)], s_in.at[pair + 1, v, :, me * halves + h]

                def send(to):
                    src, dst = part(to)
                    pltpu.make_async_remote_copy(src_ref=src, dst_ref=dst, send_sem=b_send.at[v, h], recv_sem=b_recv.at[v], device_id={"sp": to}).start()

                src, dst = part(me)
                pltpu.make_async_copy(src, dst, b_recv.at[v]).start()
                spread(send)

            @pl.when(pair == pairs - 1)
            def _():
                pltpu.make_async_copy(t_out.at[v, h], y_ref.at[v, :, h], y_sem.at[v, h]).start()

        lax.fori_loop(0, videos * halves, unit, 0)

    def run_pair(pair, carry):
        layer = 2 * pair
        wait_weights(layer, (0,))
        spatial(pair)
        wait_weights(layer + 1, range(len(weights)))

        @pl.when(pair < pairs - 1)
        def _():
            start_weights(layer + 2)

        temporal(pair)
        return carry

    lax.fori_loop(0, pairs, run_pair, 0)

    for v in range(videos):
        for h in range(halves):
            done = y_ref.at[v, :, h]
            pltpu.make_async_copy(done, done, y_sem.at[v, h]).wait()
            for pair in range(pairs):
                part = t_in.at[pair, v, h, pl.ds(0, frames - f_loc)]
                pltpu.make_async_copy(part, part, ac_send.at[pair, v, h if v else 0]).wait()


def solution(mesh):
    n = mesh.shape["sp"]

    def local_stack(x, norms, w_qkv, w_out, w_up, w_down):
        videos, f_loc, patches, width = x.shape
        layers = w_qkv.shape[0]
        pairs = layers // 2
        head = w_qkv.shape[-1]
        hidden = w_up.shape[-1]
        frames, halves = f_loc * n, patches // n // SUB
        x = x.reshape(videos, f_loc, patches // SUB, SUB, width)
        w_qkv = w_qkv.transpose(0, 2, 3, 4, 1).reshape(layers, 3 * width, width)
        w_out = w_out.reshape(layers, width, width)
        any_space = pl.BlockSpec(memory_space=pl.ANY)
        y = pl.pallas_call(
            functools.partial(kernel, n, head),
            out_shape=pltpu.VMEM((videos, frames, halves, SUB, width), BF16),
            in_specs=[any_space, pl.BlockSpec(memory_space=pltpu.VMEM)] + [any_space] * 4,
            out_specs=pl.BlockSpec(memory_space=pltpu.VMEM),
            scratch_shapes=[
                pltpu.VMEM((layers, 3 * width, width), BF16),
                pltpu.VMEM((layers, width, width), BF16),
                pltpu.VMEM((layers, width, hidden), BF16),
                pltpu.VMEM((layers, hidden, width), BF16),
                pltpu.VMEM((pairs, videos, f_loc, patches // SUB, SUB, width), BF16),
                pltpu.VMEM((pairs, videos, f_loc, patches // SUB, SUB, width), BF16),
                pltpu.VMEM((pairs, videos, halves, frames, SUB, width), BF16),
                pltpu.VMEM((videos, halves, frames, SUB, width), BF16),
                pltpu.VMEM((width // head, LANES, patches), BF16),
                pltpu.VMEM((patches, width), BF16),
                pltpu.VMEM((width, patches), BF16),
                pltpu.VMEM((width, patches), BF16),
                pltpu.VMEM((width // head, patches, patches), F32),
                pltpu.VMEM((patches, hidden), BF16),
                pltpu.VMEM((patches, width), BF16),
                pltpu.VMEM((patches, width), BF16),
                pltpu.VMEM((patches, width), BF16),
                pltpu.VMEM((patches, width), BF16),
                pltpu.VMEM((width // LANES, frames * SUB, LANES), F32),
                pltpu.VMEM((width // LANES, frames * SUB, LANES), F32),
                pltpu.VMEM((4 * frames, 4 * frames), F32),
                pltpu.SemaphoreType.DMA((layers, 4)),
                pltpu.SemaphoreType.DMA((videos,)),
                pltpu.SemaphoreType.DMA((videos,)),
                pltpu.SemaphoreType.DMA((pairs, videos, halves)),
                pltpu.SemaphoreType.DMA((videos, halves)),
                pltpu.SemaphoreType.DMA((pairs, videos, halves)),
                pltpu.SemaphoreType.DMA((videos, halves)),
            ],
            compiler_params=pltpu.CompilerParams(collective_id=0, has_side_effects=True, vmem_limit_bytes=VMEM_BYTES),
            name="stack",
        )(x, norms, w_qkv, w_out, w_up, w_down)
        return y.reshape(videos, frames, halves * SUB, width)

    replicated = P()
    return jax.shard_map(local_stack, mesh=mesh, in_specs=(P('data', 'sp', None, None), replicated, replicated, replicated, replicated, replicated), out_specs=P('data', None, 'sp', None), check_vma=False)
```

```python
import functools
import math
import jax
import jax.numpy as jnp
from jax import lax
from jax.experimental import pallas as pl
from jax.experimental.pallas import tpu as pltpu
from jax.sharding import PartitionSpec as P

EPS = 1e-6
LANES = 128
SUB = 8
VMEM_BYTES = 65_700_000
ATTENTION_STEPS, MLP_STEPS = 12, 7
GELU_A, GELU_B = math.sqrt(2 / math.pi), 0.044715
F32, BF16 = jnp.float32, jnp.bfloat16


def dot(a, b):
    return jnp.dot(a, b, preferred_element_type=F32)


def dot_nt(a, b):
    return lax.dot_general(a, b, (((1,), (1,)), ((), ())), preferred_element_type=F32)


def dot_tn(a, b):
    return lax.dot_general(a, b, (((0,), (0,)), ((), ())), preferred_element_type=F32)


def layer_norm(x, gain, shift):
    centered = x - jnp.mean(x, axis=-1, keepdims=True)
    variance = jnp.mean(centered * centered, axis=-1, keepdims=True)
    return centered * lax.rsqrt(variance + EPS) * gain + shift


def kernel(n, head, x_ref, norms, wqkv_hbm, wout_hbm, wup_hbm, wdown_hbm, y_ref,
           wqkv, wout, wup, wdown, s_in, s_out, t_in, t_out, q_s, k_s, v_s, ot_s, s_s, hid_s, next_h, next_a, cur_h, cur_a, u_f32, z_f32, mask_s,
           w_sem, x_sem, b_recv, ac_recv, b_send, ac_send):
    pairs, videos, f_loc, tiles, sub, width = s_in.shape
    halves, frames = t_in.shape[2], t_in.shape[3]
    patches = tiles * sub
    me = lax.axis_index("sp")
    pair_heads = width // LANES
    group = 4
    rows_g = group * frames
    scale = head ** -0.5

    weights = ((wqkv_hbm, wqkv), (wout_hbm, wout), (wup_hbm, wup), (wdown_hbm, wdown))

    def weight_copy(layer, i):
        src, dst = weights[i]
        return pltpu.make_async_copy(src.at[layer], dst.at[layer], w_sem.at[layer, i])

    def start_weights(layer, first=0):
        for i in range(first, len(weights)):
            weight_copy(layer, i).start()

    def wait_weights(layer, which):
        for i in which:
            weight_copy(layer, i).wait()

    pltpu.make_async_copy(x_ref.at[0], s_in.at[0, 0], x_sem.at[0]).start()
    weight_copy(0, 0).start()

    barrier = pltpu.get_barrier_semaphore()

    def tell(step, c):
        pl.semaphore_signal(barrier, inc=1, device_id={"sp": lax.rem(me + step, n)})
        return c

    lax.fori_loop(1, n, tell, 0)


    row_p = lax.broadcasted_iota(jnp.int32, (rows_g, rows_g), 0)
    col_p = lax.broadcasted_iota(jnp.int32, (rows_g, rows_g), 1)
    across = jnp.full((rows_g, rows_g), -jnp.inf, F32)
    for i in range(group):
        lo, hi = i * frames, (i + 1) * frames
        inside = (row_p >= lo) & (row_p < hi) & (col_p >= lo) & (col_p < hi)
        across = jnp.where(inside, 0.0, across)
    mask_s[...] = across
    q_s[...] = jnp.zeros_like(q_s)

    heads = width // head

    def strips(rows, masked):
        out = []
        for lo in range(0, rows, LANES):
            hi = min(rows, lo + LANES)
            out.append((lo, hi, lo // frames * frames, -(-hi // frames) * frames) if masked else (lo, hi, 0, rows))
        return out if masked else [(0, rows, 0, rows)]

    def scores(h, rows, masked):
        s = dot(k_s[pl.ds(0, rows), pl.ds(h * head // LANES * LANES, LANES)], q_s[h, :, pl.ds(0, rows)])
        tops = []
        for lo, hi, k0, k1 in strips(rows, masked):
            part = s[k0:k1, lo:hi]
            if masked:
                part = part + mask_s[pl.ds(k0, k1 - k0), pl.ds(lo, hi - lo)]
            s_s[h, pl.ds(k0, k1 - k0), pl.ds(lo, hi - lo)] = part
            tops.append(jnp.max(part, axis=0, keepdims=True) + math.log(rows))
        return tops

    def mix(h, rows, masked, tops):
        cols, sums = [], []
        for (lo, hi, k0, k1), top in zip(strips(rows, masked), tops):
            e = jnp.exp(s_s[h, pl.ds(k0, k1 - k0), pl.ds(lo, hi - lo)] - top)
            sums.append(jnp.sum(e, axis=0, keepdims=True))
            col = [jnp.zeros((k, hi - lo), BF16) for k in (k0,)] if k0 else []
            col.append(e.astype(BF16))
            if k1 < rows:
                col.append(jnp.zeros((rows - k1, hi - lo), BF16))
            cols.append(jnp.concatenate(col, axis=0) if len(col) > 1 else col[0])
        p = jnp.concatenate(cols, axis=1) if len(cols) > 1 else cols[0]
        norm = jnp.concatenate(sums, axis=1) if len(sums) > 1 else sums[0]
        o = dot(v_s[pl.ds(h * head, head), pl.ds(0, rows)], p)
        ot_s[pl.ds(h * head, head), pl.ds(0, rows)] = (o * (1.0 / norm)).astype(BF16)

    def gelu(x):
        t = jnp.tanh(x * (GELU_A + (GELU_A * GELU_B) * (x * x)))
        half = 0.5 * x
        return half + half * t

    def attention_steps(get, rows, layer, masked):
        a = layer_norm(get(), norms[layer, pl.ds(0, 1), :], norms[layer, pl.ds(1, 1), :]).astype(BF16)
        yield
        q = (dot_nt(wqkv[layer, pl.ds(0, width), :], a) * scale).astype(BF16)
        for h in range(heads):
            q_s[h, pl.ds(h * head % LANES, head), pl.ds(0, rows)] = q[h * head:(h + 1) * head]
        yield
        k_s[pl.ds(0, rows), :] = dot_nt(a, wqkv[layer, pl.ds(width, width), :]).astype(BF16)
        yield
        v_s[:, pl.ds(0, rows)] = dot_nt(wqkv[layer, pl.ds(2 * width, width), :], a).astype(BF16)
        yield
        ahead = 2
        tops = [scores(h, rows, masked) for h in range(ahead)]
        yield
        for h in range(heads):
            if h + ahead < heads:
                tops.append(scores(h + ahead, rows, masked))
            mix(h, rows, masked, tops[h])
            yield
        h = (get() + dot_tn(ot_s[:, pl.ds(0, rows)], wout[layer])).astype(BF16)
        next_h[pl.ds(0, rows), :] = h
        next_a[pl.ds(0, rows), :] = layer_norm(h.astype(F32), norms[layer, pl.ds(2, 1), :], norms[layer, pl.ds(3, 1), :]).astype(BF16)
        yield

    def mlp_steps(rows, layer, put):
        cur_h[pl.ds(0, rows), :] = next_h[pl.ds(0, rows), :]
        cur_a[pl.ds(0, rows), :] = next_a[pl.ds(0, rows), :]
        chunk = 256
        for c in range(hid_s.shape[1] // chunk):
            up = dot(cur_a[pl.ds(0, rows), :], wup[layer, :, pl.ds(c * chunk, chunk)])
            hid_s[pl.ds(0, rows), pl.ds(c * chunk, chunk)] = gelu(up).astype(BF16)
            yield
        put(cur_h[pl.ds(0, rows), :].astype(F32) + dot(hid_s[pl.ds(0, rows), :], wdown[layer]))
        yield

    def emit(first, second):
        steps = "ABAABAABAABAABAABAB" if first is not None and second is not None else "A" * ATTENTION_STEPS + "B" * MLP_STEPS
        for step in steps:
            stage = first if step == "A" else second
            if stage is not None:
                next(stage)

    def pipeline(tiles_n, attention, mlp, after, alone=None, late=None):
        steps = attention(0)
        for _ in range(ATTENTION_STEPS - 1):
            next(steps)
        if late is not None:
            late()
        next(steps)
        start = 1
        if alone is not None:
            @pl.when(alone)
            def _():
                emit(None, mlp(0))
                after(0)
                emit(attention(1), None)

            start = jnp.where(alone, 2, 1)

        def step(i, c):
            emit(attention(i), mlp(i - 1))
            after(i - 1)
            return c

        lax.fori_loop(start, tiles_n, step, 0)
        emit(None, mlp(tiles_n - 1))
        after(tiles_n - 1)

    def spread(send):
        for i in range(n // 2):
            send(lax.rem(me + n // 2 + i, n))
            if i > 0:
                send(lax.rem(me + n // 2 + n - i, n))

    def send_frame(pair, v, f):
        def part(to):
            return s_out.at[pair, v, f, pl.ds(to * halves, halves)], t_in.at[pair, v, :, me * f_loc + f]

        def send(to):
            src, dst = part(to)
            pltpu.make_async_remote_copy(src_ref=src, dst_ref=dst, send_sem=ac_send.at[pair, v, 0], recv_sem=ac_recv.at[pair, v, 0], device_id={"sp": to}).start()

        src, dst = part(me)
        pltpu.make_async_copy(src, dst, ac_recv.at[pair, v, 0]).start()
        spread(send)

    def send_half(pair, v, h):
        def part(to):
            return s_out.at[pair, v, :, to * halves + h], t_in.at[pair, v, h, pl.ds(me * f_loc, f_loc)]

        def send(to):
            src, dst = part(to)
            pltpu.make_async_remote_copy(src_ref=src, dst_ref=dst, send_sem=ac_send.at[pair, v, h], recv_sem=ac_recv.at[pair, v, h], device_id={"sp": to}).start()

        src, dst = part(me)
        pltpu.make_async_copy(src, dst, ac_recv.at[pair, v, h]).start()
        spread(send)

    def spatial(pair):
        layer = 2 * pair

        def video(v, c):
            @pl.when(pair == 0)
            def _():
                pltpu.make_async_copy(x_ref.at[v], s_in.at[0, v], x_sem.at[v]).wait()

            @pl.when(pair > 0)
            def _():
                pltpu.make_async_copy(x_ref.at[v], s_in.at[pair, v], b_recv.at[pair - 1, v]).wait()

            def attention(f):
                return attention_steps(lambda: s_in[pair, v, f].astype(F32).reshape(patches, width), patches, layer, False)

            def mlp(f):
                def put(z):
                    s_out[pair, v, f] = z.reshape(tiles, sub, width).astype(BF16)

                return mlp_steps(patches, layer, put)

            def after(f):
                @pl.when((pair == 0) & (v == 0) & (f == 0))
                def _():
                    pl.semaphore_wait(barrier, n - 1)

                @pl.when(v == 0)
                def _():
                    send_frame(pair, v, f)

                @pl.when((v > 0) & (f == f_loc - 1))
                def _():
                    for h in range(halves):
                        send_half(pair, v, h)

            def late():
                @pl.when(v == 0)
                def _():
                    wait_weights(layer, (1, 2, 3))
                    start_weights(layer + 1)

            pipeline(f_loc, attention, mlp, after, (pair == 0) & (v == 0), late)
            return c

        lax.fori_loop(0, videos, video, 0)

    def temporal(pair):
        layer = 2 * pair + 1
        groups = sub // group
        chunks = 2
        f_chunk = frames // chunks
        rows_c = f_chunk * sub

        def unit(i, carry):
            v, h = i // halves, lax.rem(i, halves)

            @pl.when((v == 0) & (h == 0))
            def _():
                pltpu.make_async_copy(t_in.at[pair, 0], t_in.at[pair, 0], ac_recv.at[pair, 0, 0]).wait()

            @pl.when(v > 0)
            def _():
                pltpu.make_async_copy(t_in.at[pair, v, h], t_in.at[pair, v, h], ac_recv.at[pair, v, h]).wait()

            def widen(c, q):
                u = t_in[pair, v, h, pl.ds(c * f_chunk, f_chunk)].astype(F32).reshape(rows_c, width)
                for j in range(pair_heads):
                    u_f32[j, pl.ds(pl.multiple_of(c * rows_c, rows_c), rows_c), :] = u[:, j * LANES:(j + 1) * LANES]
                return q

            lax.fori_loop(0, chunks, widen, 0)
            pipeline(groups, attention, mlp, lambda g: None)
            finish(v, h)
            return carry

        def attention(g):
            def get():
                return jnp.concatenate([jnp.concatenate([u_f32[j, pl.ds(g * group + p, frames, stride=sub), :] for p in range(group)], axis=0)
                                        for j in range(pair_heads)], axis=1)

            return attention_steps(get, rows_g, layer, True)

        def mlp(g):
            def put(z):
                for p in range(group):
                    for j in range(pair_heads):
                        z_f32[j, pl.ds(g * group + p, frames, stride=sub), :] = z[p * frames:(p + 1) * frames, j * LANES:(j + 1) * LANES]

            return mlp_steps(rows_g, layer, put)

        def finish(v, h):
            def narrow(c, q):
                rows = pl.ds(pl.multiple_of(c * rows_c, rows_c), rows_c)
                z = jnp.concatenate([z_f32[j, rows, :] for j in range(pair_heads)], axis=1)
                z = z.reshape(f_chunk, sub, width).astype(BF16)

                @pl.when(pair < pairs - 1)
                def _():
                    t_out[pair, v, h, pl.ds(c * f_chunk, f_chunk)] = z

                @pl.when(pair == pairs - 1)
                def _():
                    y_ref[v, pl.ds(c * f_chunk, f_chunk), h] = z
                return q

            lax.fori_loop(0, chunks, narrow, 0)

            @pl.when(pair < pairs - 1)
            def _():
                def part(to):
                    return t_out.at[pair, v, h, pl.ds(to * f_loc, f_loc)], s_in.at[pair + 1, v, :, me * halves + h]

                def send(to):
                    src, dst = part(to)
                    pltpu.make_async_remote_copy(src_ref=src, dst_ref=dst, send_sem=b_send.at[pair, v, h], recv_sem=b_recv.at[pair, v], device_id={"sp": to}).start()

                src, dst = part(me)
                pltpu.make_async_copy(src, dst, b_recv.at[pair, v]).start()
                spread(send)

        lax.fori_loop(0, videos * halves, unit, 0)

    def run_pair(pair, carry):
        layer = 2 * pair
        wait_weights(layer, (0,))

        @pl.when(pair == 0)
        def _():
            start_weights(0, 1)
            for v in range(1, videos):
                pltpu.make_async_copy(x_ref.at[v], s_in.at[0, v], x_sem.at[v]).start()

        spatial(pair)
        wait_weights(layer + 1, range(len(weights)))

        @pl.when(pair < pairs - 1)
        def _():
            start_weights(layer + 2)

        temporal(pair)
        return carry

    lax.fori_loop(0, pairs, run_pair, 0)

    for v in range(videos):
        for h in range(halves):
            part = t_in.at[0, v, h, pl.ds(0, frames - f_loc)]
            for pair in range(pairs - 1):
                pltpu.make_async_copy(part, part, b_send.at[pair, v, h]).wait()
            for pair in range(pairs):
                pltpu.make_async_copy(part, part, ac_send.at[pair, v, h if v else 0]).wait()


def solution(mesh):
    n = mesh.shape["sp"]

    def local_stack(x, norms, w_qkv, w_out, w_up, w_down):
        videos, f_loc, patches, width = x.shape
        layers = w_qkv.shape[0]
        pairs = layers // 2
        head = w_qkv.shape[-1]
        hidden = w_up.shape[-1]
        frames, halves = f_loc * n, patches // n // SUB
        x = x.reshape(videos, f_loc, patches // SUB, SUB, width)
        w_qkv = w_qkv.transpose(0, 2, 3, 4, 1).reshape(layers, 3 * width, width)
        w_out = w_out.reshape(layers, width, width)
        any_space = pl.BlockSpec(memory_space=pl.ANY)
        y = pl.pallas_call(
            functools.partial(kernel, n, head),
            out_shape=pltpu.VMEM((videos, frames, halves, SUB, width), BF16),
            in_specs=[any_space, pl.BlockSpec(memory_space=pltpu.VMEM)] + [any_space] * 4,
            out_specs=pl.BlockSpec(memory_space=pltpu.VMEM),
            scratch_shapes=[
                pltpu.VMEM((layers, 3 * width, width), BF16),
                pltpu.VMEM((layers, width, width), BF16),
                pltpu.VMEM((layers, width, hidden), BF16),
                pltpu.VMEM((layers, hidden, width), BF16),
                pltpu.VMEM((pairs, videos, f_loc, patches // SUB, SUB, width), BF16),
                pltpu.VMEM((pairs, videos, f_loc, patches // SUB, SUB, width), BF16),
                pltpu.VMEM((pairs, videos, halves, frames, SUB, width), BF16),
                pltpu.VMEM((pairs - 1, videos, halves, frames, SUB, width), BF16),
                pltpu.VMEM((width // head, LANES, patches), BF16),
                pltpu.VMEM((patches, width), BF16),
                pltpu.VMEM((width, patches), BF16),
                pltpu.VMEM((width, patches), BF16),
                pltpu.VMEM((width // head, patches, patches), F32),
                pltpu.VMEM((patches, hidden), BF16),
                pltpu.VMEM((patches, width), BF16),
                pltpu.VMEM((patches, width), BF16),
                pltpu.VMEM((patches, width), BF16),
                pltpu.VMEM((patches, width), BF16),
                pltpu.VMEM((width // LANES, frames * SUB, LANES), F32),
                pltpu.VMEM((width // LANES, frames * SUB, LANES), F32),
                pltpu.VMEM((4 * frames, 4 * frames), F32),
                pltpu.SemaphoreType.DMA((layers, 4)),
                pltpu.SemaphoreType.DMA((videos,)),
                pltpu.SemaphoreType.DMA((pairs - 1, videos)),
                pltpu.SemaphoreType.DMA((pairs, videos, halves)),
                pltpu.SemaphoreType.DMA((pairs - 1, videos, halves)),
                pltpu.SemaphoreType.DMA((pairs, videos, halves)),
            ],
            compiler_params=pltpu.CompilerParams(collective_id=0, has_side_effects=True, vmem_limit_bytes=VMEM_BYTES),
            name="stack",
        )(x, norms, w_qkv, w_out, w_up, w_down)
        return y.reshape(videos, frames, halves * SUB, width)

    replicated = P()
    return jax.shard_map(local_stack, mesh=mesh, in_specs=(P('data', 'sp', None, None), replicated, replicated, replicated, replicated, replicated), out_specs=P('data', None, 'sp', None), check_vma=False)
```

```python
import functools
import math
import jax
import jax.numpy as jnp
from jax import lax
from jax.experimental import pallas as pl
from jax.experimental.pallas import tpu as pltpu
from jax.sharding import PartitionSpec as P

EPS = 1e-6
LANES = 128
SUB = 8
VMEM_BYTES = 65_700_000
ATTENTION_STEPS, MLP_STEPS = 12, 7
UNIT_ORDER = "aaaaa" "abababababa" "bb" "a" "bbb" "cbcc" "b" "cccc" "ddddddd"
GELU_A, GELU_B = math.sqrt(2 / math.pi), 0.044715
F32, BF16 = jnp.float32, jnp.bfloat16


def dot(a, b):
    return jnp.dot(a, b, preferred_element_type=F32)


def dot_nt(a, b):
    return lax.dot_general(a, b, (((1,), (1,)), ((), ())), preferred_element_type=F32)


def dot_tn(a, b):
    return lax.dot_general(a, b, (((0,), (0,)), ((), ())), preferred_element_type=F32)


def layer_norm(x, gain, shift):
    centered = x - jnp.mean(x, axis=-1, keepdims=True)
    variance = jnp.mean(centered * centered, axis=-1, keepdims=True)
    return centered * lax.rsqrt(variance + EPS) * gain + shift


def kernel(n, head, x_ref, norms, wqkv_hbm, wout_hbm, wup_hbm, wdown_hbm, y_ref,
           wqkv, wout, wup, wdown, s_in, s_out, t_in, t_out, q_s, k_s, v_s, ot_s, s_s, hid_s, next_h, next_a, cur_h, cur_a, u_f32, z_f32, mask_s,
           w_sem, x_sem, b_recv, ac_recv, b_send, ac_send):
    pairs, videos, f_loc, tiles, sub, width = s_in.shape
    halves, frames = t_in.shape[2], t_in.shape[3]
    patches = tiles * sub
    me = lax.axis_index("sp")
    pair_heads = width // LANES
    group = 4
    rows_g = group * frames
    scale = head ** -0.5

    weights = ((wqkv_hbm, wqkv), (wout_hbm, wout), (wup_hbm, wup), (wdown_hbm, wdown))

    def weight_copy(layer, i):
        src, dst = weights[i]
        return pltpu.make_async_copy(src.at[layer], dst.at[layer], w_sem.at[layer, i])

    def start_weights(layer, first=0):
        for i in range(first, len(weights)):
            weight_copy(layer, i).start()

    def wait_weights(layer, which):
        for i in which:
            weight_copy(layer, i).wait()

    pltpu.make_async_copy(x_ref.at[0], s_in.at[0, 0], x_sem.at[0]).start()
    weight_copy(0, 0).start()

    barrier = pltpu.get_barrier_semaphore()

    def tell(step, c):
        pl.semaphore_signal(barrier, inc=1, device_id={"sp": lax.rem(me + step, n)})
        return c

    lax.fori_loop(1, n, tell, 0)


    row_p = lax.broadcasted_iota(jnp.int32, (rows_g, rows_g), 0)
    col_p = lax.broadcasted_iota(jnp.int32, (rows_g, rows_g), 1)
    across = jnp.full((rows_g, rows_g), -jnp.inf, F32)
    for i in range(group):
        lo, hi = i * frames, (i + 1) * frames
        inside = (row_p >= lo) & (row_p < hi) & (col_p >= lo) & (col_p < hi)
        across = jnp.where(inside, 0.0, across)
    mask_s[...] = across
    q_s[...] = jnp.zeros_like(q_s)

    heads = width // head

    def strips(rows, masked):
        out = []
        for lo in range(0, rows, LANES):
            hi = min(rows, lo + LANES)
            out.append((lo, hi, lo // frames * frames, -(-hi // frames) * frames) if masked else (lo, hi, 0, rows))
        return out if masked else [(0, rows, 0, rows)]

    def scores(par, h, rows, masked):
        s = dot(k_s[par, pl.ds(0, rows), pl.ds(h * head // LANES * LANES, LANES)], q_s[par, h, :, pl.ds(0, rows)])
        tops = []
        for lo, hi, k0, k1 in strips(rows, masked):
            part = s[k0:k1, lo:hi]
            if masked:
                part = part + mask_s[pl.ds(k0, k1 - k0), pl.ds(lo, hi - lo)]
            s_s[par, h, pl.ds(k0, k1 - k0), pl.ds(lo, hi - lo)] = part
            tops.append(jnp.max(part, axis=0, keepdims=True) + math.log(rows))
        return tops

    def mix(par, h, rows, masked, tops):
        cols, sums = [], []
        for (lo, hi, k0, k1), top in zip(strips(rows, masked), tops):
            e = jnp.exp(s_s[par, h, pl.ds(k0, k1 - k0), pl.ds(lo, hi - lo)] - top)
            sums.append(jnp.sum(e, axis=0, keepdims=True))
            col = [jnp.zeros((k, hi - lo), BF16) for k in (k0,)] if k0 else []
            col.append(e.astype(BF16))
            if k1 < rows:
                col.append(jnp.zeros((rows - k1, hi - lo), BF16))
            cols.append(jnp.concatenate(col, axis=0) if len(col) > 1 else col[0])
        p = jnp.concatenate(cols, axis=1) if len(cols) > 1 else cols[0]
        norm = jnp.concatenate(sums, axis=1) if len(sums) > 1 else sums[0]
        o = dot(v_s[par, pl.ds(h * head, head), pl.ds(0, rows)], p)
        ot_s[par, pl.ds(h * head, head), pl.ds(0, rows)] = (o * (1.0 / norm)).astype(BF16)

    def gelu(x):
        t = jnp.tanh(x * (GELU_A + (GELU_A * GELU_B) * (x * x)))
        half = 0.5 * x
        return half + half * t

    def attention_steps(get, rows, layer, masked, par=0):
        a = layer_norm(get(), norms[layer, pl.ds(0, 1), :], norms[layer, pl.ds(1, 1), :]).astype(BF16)
        yield
        q = (dot_nt(wqkv[layer, pl.ds(0, width), :], a) * scale).astype(BF16)
        for h in range(heads):
            q_s[par, h, pl.ds(h * head % LANES, head), pl.ds(0, rows)] = q[h * head:(h + 1) * head]
        yield
        k_s[par, pl.ds(0, rows), :] = dot_nt(a, wqkv[layer, pl.ds(width, width), :]).astype(BF16)
        yield
        v_s[par, :, pl.ds(0, rows)] = dot_nt(wqkv[layer, pl.ds(2 * width, width), :], a).astype(BF16)
        yield
        ahead = 2
        tops = [scores(par, h, rows, masked) for h in range(ahead)]
        yield
        for h in range(heads):
            if h + ahead < heads:
                tops.append(scores(par, h + ahead, rows, masked))
            mix(par, h, rows, masked, tops[h])
            yield
        h = (get() + dot_tn(ot_s[par, :, pl.ds(0, rows)], wout[layer])).astype(BF16)
        next_h[par, pl.ds(0, rows), :] = h
        next_a[par, pl.ds(0, rows), :] = layer_norm(h.astype(F32), norms[layer, pl.ds(2, 1), :], norms[layer, pl.ds(3, 1), :]).astype(BF16)
        yield

    def mlp_steps(rows, layer, put, par=None):
        if par is None:
            cur_h[pl.ds(0, rows), :] = next_h[0, pl.ds(0, rows), :]
            cur_a[pl.ds(0, rows), :] = next_a[0, pl.ds(0, rows), :]
            h_ref, a_ref, par = cur_h, cur_a, 0
        else:
            h_ref, a_ref = next_h.at[par], next_a.at[par]
        chunk = 256
        for c in range(hid_s.shape[2] // chunk):
            up = dot(a_ref[pl.ds(0, rows), :], wup[layer, :, pl.ds(c * chunk, chunk)])
            hid_s[par, pl.ds(0, rows), pl.ds(c * chunk, chunk)] = gelu(up).astype(BF16)
            yield
        put(h_ref[pl.ds(0, rows), :].astype(F32) + dot(hid_s[par, pl.ds(0, rows), :], wdown[layer]))
        yield

    def emit(first, second):
        steps = "ABAABAABAABAABAABAB" if first is not None and second is not None else "A" * ATTENTION_STEPS + "B" * MLP_STEPS
        for step in steps:
            stage = first if step == "A" else second
            if stage is not None:
                next(stage)

    def pipeline(tiles_n, attention, mlp, after, alone=None, late=None):
        steps = attention(0)
        for _ in range(ATTENTION_STEPS - 1):
            next(steps)
        if late is not None:
            late()
        next(steps)
        start = 1
        if alone is not None:
            @pl.when(alone)
            def _():
                emit(None, mlp(0))
                after(0)
                emit(attention(1), None)

            start = jnp.where(alone, 2, 1)

        def step(i, c):
            emit(attention(i), mlp(i - 1))
            after(i - 1)
            return c

        lax.fori_loop(start, tiles_n, step, 0)
        emit(None, mlp(tiles_n - 1))
        after(tiles_n - 1)

    def spread(send):
        for i in range(n // 2):
            send(lax.rem(me + n // 2 + i, n))
            if i > 0:
                send(lax.rem(me + n // 2 + n - i, n))

    def send_frame(pair, v, f):
        def part(to):
            return s_out.at[pair, v, f, pl.ds(to * halves, halves)], t_in.at[pair, v, :, me * f_loc + f]

        def send(to):
            src, dst = part(to)
            pltpu.make_async_remote_copy(src_ref=src, dst_ref=dst, send_sem=ac_send.at[pair, v, 0], recv_sem=ac_recv.at[pair, v, 0], device_id={"sp": to}).start()

        src, dst = part(me)
        pltpu.make_async_copy(src, dst, ac_recv.at[pair, v, 0]).start()
        spread(send)

    def send_half(pair, v, h):
        def part(to):
            return s_out.at[pair, v, :, to * halves + h], t_in.at[pair, v, h, pl.ds(me * f_loc, f_loc)]

        def send(to):
            src, dst = part(to)
            pltpu.make_async_remote_copy(src_ref=src, dst_ref=dst, send_sem=ac_send.at[pair, v, h], recv_sem=ac_recv.at[pair, v, h], device_id={"sp": to}).start()

        src, dst = part(me)
        pltpu.make_async_copy(src, dst, ac_recv.at[pair, v, h]).start()
        spread(send)

    def spatial(pair):
        layer = 2 * pair

        def video(v, c):
            @pl.when(pair == 0)
            def _():
                pltpu.make_async_copy(x_ref.at[v], s_in.at[0, v], x_sem.at[v]).wait()

            @pl.when(pair > 0)
            def _():
                pltpu.make_async_copy(x_ref.at[v], s_in.at[pair, v], b_recv.at[pair - 1, v]).wait()

            def attention(f):
                return attention_steps(lambda: s_in[pair, v, f].astype(F32).reshape(patches, width), patches, layer, False)

            def mlp(f):
                def put(z):
                    s_out[pair, v, f] = z.reshape(tiles, sub, width).astype(BF16)

                return mlp_steps(patches, layer, put)

            def after(f):
                @pl.when((pair == 0) & (v == 0) & (f == 0))
                def _():
                    pl.semaphore_wait(barrier, n - 1)

                @pl.when(v == 0)
                def _():
                    send_frame(pair, v, f)

                @pl.when((v > 0) & (f == f_loc - 1))
                def _():
                    for h in range(halves):
                        send_half(pair, v, h)

            def late():
                @pl.when(v == 0)
                def _():
                    wait_weights(layer, (1, 2, 3))
                    start_weights(layer + 1)

            pipeline(f_loc, attention, mlp, after, (pair == 0) & (v == 0), late)
            return c

        lax.fori_loop(0, videos, video, 0)

    def temporal(pair):
        layer = 2 * pair + 1
        groups = sub // group
        chunks = 2
        f_chunk = frames // chunks
        rows_c = f_chunk * sub

        def unit(i, carry):
            v, h = i // halves, lax.rem(i, halves)

            @pl.when((v == 0) & (h == 0))
            def _():
                pltpu.make_async_copy(t_in.at[pair, 0], t_in.at[pair, 0], ac_recv.at[pair, 0, 0]).wait()

            @pl.when(v > 0)
            def _():
                pltpu.make_async_copy(t_in.at[pair, v, h], t_in.at[pair, v, h], ac_recv.at[pair, v, h]).wait()

            def widen(c, q):
                u = t_in[pair, v, h, pl.ds(c * f_chunk, f_chunk)].astype(F32).reshape(rows_c, width)
                for j in range(pair_heads):
                    u_f32[j, pl.ds(pl.multiple_of(c * rows_c, rows_c), rows_c), :] = u[:, j * LANES:(j + 1) * LANES]
                return q

            lax.fori_loop(0, chunks, widen, 0)
            streams = {"a": attention(0), "b": attention(1), "c": mlp(0), "d": mlp(1)}
            for step in UNIT_ORDER:
                next(streams[step])
            finish(v, h)
            return carry

        def attention(g):
            def get():
                return jnp.concatenate([jnp.concatenate([u_f32[j, pl.ds(g * group + p, frames, stride=sub), :] for p in range(group)], axis=0)
                                        for j in range(pair_heads)], axis=1)

            return attention_steps(get, rows_g, layer, True, g)

        def mlp(g):
            def put(z):
                for p in range(group):
                    for j in range(pair_heads):
                        z_f32[j, pl.ds(g * group + p, frames, stride=sub), :] = z[p * frames:(p + 1) * frames, j * LANES:(j + 1) * LANES]

            return mlp_steps(rows_g, layer, put, g)

        def finish(v, h):
            def narrow(c, q):
                rows = pl.ds(pl.multiple_of(c * rows_c, rows_c), rows_c)
                z = jnp.concatenate([z_f32[j, rows, :] for j in range(pair_heads)], axis=1)
                z = z.reshape(f_chunk, sub, width).astype(BF16)

                @pl.when(pair < pairs - 1)
                def _():
                    t_out[pair, v, h, pl.ds(c * f_chunk, f_chunk)] = z

                @pl.when(pair == pairs - 1)
                def _():
                    y_ref[v, pl.ds(c * f_chunk, f_chunk), h] = z
                return q

            lax.fori_loop(0, chunks, narrow, 0)

            @pl.when(pair < pairs - 1)
            def _():
                def part(to):
                    return t_out.at[pair, v, h, pl.ds(to * f_loc, f_loc)], s_in.at[pair + 1, v, :, me * halves + h]

                def send(to):
                    src, dst = part(to)
                    pltpu.make_async_remote_copy(src_ref=src, dst_ref=dst, send_sem=b_send.at[pair, v, h], recv_sem=b_recv.at[pair, v], device_id={"sp": to}).start()

                src, dst = part(me)
                pltpu.make_async_copy(src, dst, b_recv.at[pair, v]).start()
                spread(send)

        lax.fori_loop(0, videos * halves, unit, 0)

    def run_pair(pair, carry):
        layer = 2 * pair
        wait_weights(layer, (0,))

        @pl.when(pair == 0)
        def _():
            start_weights(0, 1)
            for v in range(1, videos):
                pltpu.make_async_copy(x_ref.at[v], s_in.at[0, v], x_sem.at[v]).start()

        spatial(pair)
        wait_weights(layer + 1, range(len(weights)))

        @pl.when(pair < pairs - 1)
        def _():
            start_weights(layer + 2)

        temporal(pair)
        return carry

    lax.fori_loop(0, pairs, run_pair, 0)

    for v in range(videos):
        for h in range(halves):
            part = t_in.at[0, v, h, pl.ds(0, frames - f_loc)]
            for pair in range(pairs - 1):
                pltpu.make_async_copy(part, part, b_send.at[pair, v, h]).wait()
            for pair in range(pairs):
                pltpu.make_async_copy(part, part, ac_send.at[pair, v, h if v else 0]).wait()


def solution(mesh):
    n = mesh.shape["sp"]

    def local_stack(x, norms, w_qkv, w_out, w_up, w_down):
        videos, f_loc, patches, width = x.shape
        layers = w_qkv.shape[0]
        pairs = layers // 2
        head = w_qkv.shape[-1]
        hidden = w_up.shape[-1]
        frames, halves = f_loc * n, patches // n // SUB
        x = x.reshape(videos, f_loc, patches // SUB, SUB, width)
        w_qkv = w_qkv.transpose(0, 2, 3, 4, 1).reshape(layers, 3 * width, width)
        w_out = w_out.reshape(layers, width, width)
        any_space = pl.BlockSpec(memory_space=pl.ANY)
        y = pl.pallas_call(
            functools.partial(kernel, n, head),
            out_shape=pltpu.VMEM((videos, frames, halves, SUB, width), BF16),
            in_specs=[any_space, pl.BlockSpec(memory_space=pltpu.VMEM)] + [any_space] * 4,
            out_specs=pl.BlockSpec(memory_space=pltpu.VMEM),
            scratch_shapes=[
                pltpu.VMEM((layers, 3 * width, width), BF16),
                pltpu.VMEM((layers, width, width), BF16),
                pltpu.VMEM((layers, width, hidden), BF16),
                pltpu.VMEM((layers, hidden, width), BF16),
                pltpu.VMEM((pairs, videos, f_loc, patches // SUB, SUB, width), BF16),
                pltpu.VMEM((pairs, videos, f_loc, patches // SUB, SUB, width), BF16),
                pltpu.VMEM((pairs, videos, halves, frames, SUB, width), BF16),
                pltpu.VMEM((pairs - 1, videos, halves, frames, SUB, width), BF16),
                pltpu.VMEM((2, width // head, LANES, patches), BF16),
                pltpu.VMEM((2, patches, width), BF16),
                pltpu.VMEM((2, width, patches), BF16),
                pltpu.VMEM((2, width, patches), BF16),
                pltpu.VMEM((2, width // head, patches, patches), F32),
                pltpu.VMEM((2, patches, hidden), BF16),
                pltpu.VMEM((2, patches, width), BF16),
                pltpu.VMEM((2, patches, width), BF16),
                pltpu.VMEM((patches, width), BF16),
                pltpu.VMEM((patches, width), BF16),
                pltpu.VMEM((width // LANES, frames * SUB, LANES), F32),
                pltpu.VMEM((width // LANES, frames * SUB, LANES), F32),
                pltpu.VMEM((4 * frames, 4 * frames), F32),
                pltpu.SemaphoreType.DMA((layers, 4)),
                pltpu.SemaphoreType.DMA((videos,)),
                pltpu.SemaphoreType.DMA((pairs - 1, videos)),
                pltpu.SemaphoreType.DMA((pairs, videos, halves)),
                pltpu.SemaphoreType.DMA((pairs - 1, videos, halves)),
                pltpu.SemaphoreType.DMA((pairs, videos, halves)),
            ],
            compiler_params=pltpu.CompilerParams(collective_id=0, has_side_effects=True, vmem_limit_bytes=VMEM_BYTES),
            name="stack",
        )(x, norms, w_qkv, w_out, w_up, w_down)
        return y.reshape(videos, frames, halves * SUB, width)

    replicated = P()
    return jax.shard_map(local_stack, mesh=mesh, in_specs=(P('data', 'sp', None, None), replicated, replicated, replicated, replicated, replicated), out_specs=P('data', None, 'sp', None), check_vma=False)
```

```python
import functools
import math
import jax
import jax.numpy as jnp
from jax import lax
from jax.experimental import pallas as pl
from jax.experimental.pallas import tpu as pltpu
from jax.sharding import PartitionSpec as P

EPS = 1e-6
LANES = 128
SUB = 8
VMEM_BYTES = 65_700_000
ATTENTION_STEPS, MLP_STEPS = 12, 7
UNIT_ORDER = "aaaaa" "abababababa" "bb" "a" "bbb" "cbcc" "b" "cccc" "ddddddd"
GELU_A, GELU_B = math.sqrt(2 / math.pi), 0.044715
F32, BF16 = jnp.float32, jnp.bfloat16


def dot(a, b):
    return jnp.dot(a, b, preferred_element_type=F32)


def dot_nt(a, b):
    return lax.dot_general(a, b, (((1,), (1,)), ((), ())), preferred_element_type=F32)


def dot_tn(a, b):
    return lax.dot_general(a, b, (((0,), (0,)), ((), ())), preferred_element_type=F32)


def layer_norm(x, gain, shift):
    centered = x - jnp.mean(x, axis=-1, keepdims=True)
    variance = jnp.mean(centered * centered, axis=-1, keepdims=True)
    return centered * lax.rsqrt(variance + EPS) * gain + shift


def kernel(n, head, x_ref, norms, wqkv_hbm, wout_hbm, wup_hbm, wdown_hbm, y_ref,
           wqkv, wout, wup, wdown, s_in, s_out, t_in, t_out, q_s, k_s, v_s, ot_s, s_s, hid_s, next_h, next_a, cur_h, cur_a, u_f32, z_f32, mask_s,
           w_sem, x_sem, b_recv, ac_recv, b_send, ac_send):
    pairs, videos, f_loc, tiles, sub, width = s_in.shape
    halves, frames = t_in.shape[2], t_in.shape[3]
    patches = tiles * sub
    me = lax.axis_index("sp")
    pair_heads = width // LANES
    group = 4
    rows_g = group * frames
    scale = head ** -0.5

    weights = ((wqkv_hbm, wqkv), (wout_hbm, wout), (wup_hbm, wup), (wdown_hbm, wdown))

    def weight_copy(layer, i):
        src, dst = weights[i]
        return pltpu.make_async_copy(src.at[layer], dst.at[layer], w_sem.at[layer, i])

    def start_weights(layer, first=0):
        for i in range(first, len(weights)):
            weight_copy(layer, i).start()

    def wait_weights(layer, which):
        for i in which:
            weight_copy(layer, i).wait()

    pltpu.make_async_copy(x_ref.at[0], s_in.at[0, 0], x_sem.at[0]).start()
    weight_copy(0, 0).start()

    barrier = pltpu.get_barrier_semaphore()

    def tell(step, c):
        pl.semaphore_signal(barrier, inc=1, device_id={"sp": lax.rem(me + step, n)})
        return c

    lax.fori_loop(1, n, tell, 0)


    row_p = lax.broadcasted_iota(jnp.int32, (rows_g, rows_g), 0)
    col_p = lax.broadcasted_iota(jnp.int32, (rows_g, rows_g), 1)
    across = jnp.full((rows_g, rows_g), -jnp.inf, F32)
    for i in range(group):
        lo, hi = i * frames, (i + 1) * frames
        inside = (row_p >= lo) & (row_p < hi) & (col_p >= lo) & (col_p < hi)
        across = jnp.where(inside, 0.0, across)
    mask_s[...] = across
    q_s[...] = jnp.zeros_like(q_s)

    heads = width // head

    def strips(rows, masked):
        out = []
        for lo in range(0, rows, LANES):
            hi = min(rows, lo + LANES)
            out.append((lo, hi, lo // frames * frames, -(-hi // frames) * frames) if masked else (lo, hi, 0, rows))
        return out if masked else [(0, rows, 0, rows)]

    def scores(par, h, rows, masked):
        s = dot(k_s[par, pl.ds(0, rows), pl.ds(h * head // LANES * LANES, LANES)], q_s[par, h, :, pl.ds(0, rows)])
        tops = []
        for lo, hi, k0, k1 in strips(rows, masked):
            part = s[k0:k1, lo:hi]
            if masked:
                part = part + mask_s[pl.ds(k0, k1 - k0), pl.ds(lo, hi - lo)]
            s_s[par, h, pl.ds(k0, k1 - k0), pl.ds(lo, hi - lo)] = part
            tops.append(jnp.max(part, axis=0, keepdims=True) + math.log(rows))
        return tops

    def mix(par, h, rows, masked, tops):
        cols, sums = [], []
        for (lo, hi, k0, k1), top in zip(strips(rows, masked), tops):
            e = jnp.exp(s_s[par, h, pl.ds(k0, k1 - k0), pl.ds(lo, hi - lo)] - top)
            sums.append(jnp.sum(e, axis=0, keepdims=True))
            col = [jnp.zeros((k, hi - lo), BF16) for k in (k0,)] if k0 else []
            col.append(e.astype(BF16))
            if k1 < rows:
                col.append(jnp.zeros((rows - k1, hi - lo), BF16))
            cols.append(jnp.concatenate(col, axis=0) if len(col) > 1 else col[0])
        p = jnp.concatenate(cols, axis=1) if len(cols) > 1 else cols[0]
        norm = jnp.concatenate(sums, axis=1) if len(sums) > 1 else sums[0]
        o = dot(v_s[par, pl.ds(h * head, head), pl.ds(0, rows)], p)
        ot_s[par, pl.ds(h * head, head), pl.ds(0, rows)] = (o * (1.0 / norm)).astype(BF16)

    def gelu(x):
        t = jnp.tanh(x * (GELU_A + (GELU_A * GELU_B) * (x * x)))
        half = 0.5 * x
        return half + half * t

    def attention_steps(get, rows, layer, masked, par=0):
        a = layer_norm(get(), norms[layer, pl.ds(0, 1), :], norms[layer, pl.ds(1, 1), :]).astype(BF16)
        yield
        q = (dot_nt(wqkv[layer, pl.ds(0, width), :], a) * scale).astype(BF16)
        for h in range(heads):
            q_s[par, h, pl.ds(h * head % LANES, head), pl.ds(0, rows)] = q[h * head:(h + 1) * head]
        yield
        k_s[par, pl.ds(0, rows), :] = dot_nt(a, wqkv[layer, pl.ds(width, width), :]).astype(BF16)
        yield
        v_s[par, :, pl.ds(0, rows)] = dot_nt(wqkv[layer, pl.ds(2 * width, width), :], a).astype(BF16)
        yield
        ahead = 2
        tops = [scores(par, h, rows, masked) for h in range(ahead)]
        yield
        for h in range(heads):
            if h + ahead < heads:
                tops.append(scores(par, h + ahead, rows, masked))
            mix(par, h, rows, masked, tops[h])
            yield
        h = (get() + dot_tn(ot_s[par, :, pl.ds(0, rows)], wout[layer])).astype(BF16)
        next_h[par, pl.ds(0, rows), :] = h
        next_a[par, pl.ds(0, rows), :] = layer_norm(h.astype(F32), norms[layer, pl.ds(2, 1), :], norms[layer, pl.ds(3, 1), :]).astype(BF16)
        yield

    def mlp_steps(rows, layer, put, par=None, row0=0):
        if par is None:
            cur_h[pl.ds(0, rows), :] = next_h[0, pl.ds(0, rows), :]
            cur_a[pl.ds(0, rows), :] = next_a[0, pl.ds(0, rows), :]
            h_ref, a_ref, par = cur_h, cur_a, 0
        else:
            h_ref, a_ref = next_h.at[par], next_a.at[par]
        chunk = 256
        for c in range(hid_s.shape[2] // chunk):
            up = dot(a_ref[pl.ds(row0, rows), :], wup[layer, :, pl.ds(c * chunk, chunk)])
            hid_s[par, pl.ds(0, rows), pl.ds(c * chunk, chunk)] = gelu(up).astype(BF16)
            yield
        put(h_ref[pl.ds(row0, rows), :].astype(F32) + dot(hid_s[par, pl.ds(0, rows), :], wdown[layer]))
        yield

    def emit(first, second):
        steps = "ABAABAABAABAABAABAB" if first is not None and second is not None else "A" * ATTENTION_STEPS + "B" * MLP_STEPS
        for step in steps:
            stage = first if step == "A" else second
            if stage is not None:
                next(stage)

    def pipeline(tiles_n, attention, mlp, after, alone, first, late):
        steps = attention(0)
        for _ in range(ATTENTION_STEPS - 1):
            next(steps)
        late()
        next(steps)

        @pl.when(alone)
        def _():
            first()
            emit(attention(1), None)

        start = jnp.where(alone, 2, 1)

        def step(i, c):
            emit(attention(i), mlp(i - 1))
            after(i - 1)
            return c

        lax.fori_loop(start, tiles_n, step, 0)
        emit(None, mlp(tiles_n - 1))
        after(tiles_n - 1)

    def spread(send):
        for i in range(n // 2):
            send(lax.rem(me + n // 2 + i, n))
            if i > 0:
                send(lax.rem(me + n // 2 + n - i, n))

    def send_frame(pair, v, f):
        def part(to):
            return s_out.at[pair, v, f, pl.ds(to * halves, halves)], t_in.at[pair, v, :, me * f_loc + f]

        def send(to):
            src, dst = part(to)
            pltpu.make_async_remote_copy(src_ref=src, dst_ref=dst, send_sem=ac_send.at[pair, v, 0], recv_sem=ac_recv.at[pair, v, 0], device_id={"sp": to}).start()

        src, dst = part(me)
        pltpu.make_async_copy(src, dst, ac_recv.at[pair, v, 0]).start()
        spread(send)

    def send_half(pair, v, h):
        def part(to):
            return s_out.at[pair, v, :, to * halves + h], t_in.at[pair, v, h, pl.ds(me * f_loc, f_loc)]

        def send(to):
            src, dst = part(to)
            pltpu.make_async_remote_copy(src_ref=src, dst_ref=dst, send_sem=ac_send.at[pair, v, h], recv_sem=ac_recv.at[pair, v, h], device_id={"sp": to}).start()

        src, dst = part(me)
        pltpu.make_async_copy(src, dst, ac_recv.at[pair, v, h]).start()
        spread(send)

    def spatial(pair):
        layer = 2 * pair

        def video(v, c):
            @pl.when(pair == 0)
            def _():
                pltpu.make_async_copy(x_ref.at[v], s_in.at[0, v], x_sem.at[v]).wait()

            @pl.when(pair > 0)
            def _():
                pltpu.make_async_copy(x_ref.at[v], s_in.at[pair, v], b_recv.at[pair - 1, v]).wait()

            def attention(f):
                return attention_steps(lambda: s_in[pair, v, f].astype(F32).reshape(patches, width), patches, layer, False)

            def mlp(f):
                def put(z):
                    s_out[pair, v, f] = z.reshape(tiles, sub, width).astype(BF16)

                return mlp_steps(patches, layer, put)

            def after(f):
                @pl.when(v == 0)
                def _():
                    send_frame(pair, v, f)

                @pl.when((v > 0) & (f == f_loc - 1))
                def _():
                    for h in range(halves):
                        send_half(pair, v, h)

            def late():
                @pl.when(v == 0)
                def _():
                    wait_weights(layer, (1, 2, 3))
                    start_weights(layer + 1)

            def first():
                rows, cut = patches // 2, tiles // 2

                def part(to):
                    return s_out.at[pair, v, 0, pl.ds(to * halves, halves)], t_in.at[pair, v, :, me * f_loc]

                def rows_of(r, q):
                    def put(z):
                        s_out[pair, v, 0, pl.ds(r * cut, cut)] = z.reshape(cut, sub, width).astype(BF16)

                    emit(None, mlp_steps(rows, layer, put, 0, pl.multiple_of(r * rows, rows)))

                    @pl.when(r == 0)
                    def _():
                        pl.semaphore_wait(barrier, n - 1)

                    for i in range(n // 2):
                        to = r * (n // 2) + lax.rem(me + n // 4 + i, n // 2)

                        @pl.when(to != me)
                        def _():
                            src, dst = part(to)
                            pltpu.make_async_remote_copy(src_ref=src, dst_ref=dst, send_sem=ac_send.at[pair, v, 0], recv_sem=ac_recv.at[pair, v, 0], device_id={"sp": to}).start()
                    return q

                lax.fori_loop(0, 2, rows_of, 0)
                src, dst = part(me)
                pltpu.make_async_copy(src, dst, ac_recv.at[pair, v, 0]).start()

            pipeline(f_loc, attention, mlp, after, (pair == 0) & (v == 0), first, late)
            return c

        lax.fori_loop(0, videos, video, 0)

    def temporal(pair):
        layer = 2 * pair + 1
        groups = sub // group
        chunks = 2
        f_chunk = frames // chunks
        rows_c = f_chunk * sub

        def unit(i, carry):
            v, h = i // halves, lax.rem(i, halves)

            @pl.when((v == 0) & (h == 0))
            def _():
                pltpu.make_async_copy(t_in.at[pair, 0], t_in.at[pair, 0], ac_recv.at[pair, 0, 0]).wait()

            @pl.when(v > 0)
            def _():
                pltpu.make_async_copy(t_in.at[pair, v, h], t_in.at[pair, v, h], ac_recv.at[pair, v, h]).wait()

            def widen(c, q):
                u = t_in[pair, v, h, pl.ds(c * f_chunk, f_chunk)].astype(F32).reshape(rows_c, width)
                for j in range(pair_heads):
                    u_f32[j, pl.ds(pl.multiple_of(c * rows_c, rows_c), rows_c), :] = u[:, j * LANES:(j + 1) * LANES]
                return q

            lax.fori_loop(0, chunks, widen, 0)
            streams = {"a": attention(0), "b": attention(1), "c": mlp(0), "d": mlp(1)}
            for step in UNIT_ORDER:
                next(streams[step])
            finish(v, h)
            return carry

        def attention(g):
            def get():
                return jnp.concatenate([jnp.concatenate([u_f32[j, pl.ds(g * group + p, frames, stride=sub), :] for p in range(group)], axis=0)
                                        for j in range(pair_heads)], axis=1)

            return attention_steps(get, rows_g, layer, True, g)

        def mlp(g):
            def put(z):
                for p in range(group):
                    for j in range(pair_heads):
                        z_f32[j, pl.ds(g * group + p, frames, stride=sub), :] = z[p * frames:(p + 1) * frames, j * LANES:(j + 1) * LANES]

            return mlp_steps(rows_g, layer, put, g)

        def finish(v, h):
            def narrow(c, q):
                rows = pl.ds(pl.multiple_of(c * rows_c, rows_c), rows_c)
                z = jnp.concatenate([z_f32[j, rows, :] for j in range(pair_heads)], axis=1)
                z = z.reshape(f_chunk, sub, width).astype(BF16)

                @pl.when(pair < pairs - 1)
                def _():
                    t_out[pair, v, h, pl.ds(c * f_chunk, f_chunk)] = z

                @pl.when(pair == pairs - 1)
                def _():
                    y_ref[v, pl.ds(c * f_chunk, f_chunk), h] = z
                return q

            lax.fori_loop(0, chunks, narrow, 0)

            @pl.when(pair < pairs - 1)
            def _():
                def part(to):
                    return t_out.at[pair, v, h, pl.ds(to * f_loc, f_loc)], s_in.at[pair + 1, v, :, me * halves + h]

                def send(to):
                    src, dst = part(to)
                    pltpu.make_async_remote_copy(src_ref=src, dst_ref=dst, send_sem=b_send.at[pair, v, h], recv_sem=b_recv.at[pair, v], device_id={"sp": to}).start()

                src, dst = part(me)
                pltpu.make_async_copy(src, dst, b_recv.at[pair, v]).start()
                spread(send)

        lax.fori_loop(0, videos * halves, unit, 0)

    def run_pair(pair, carry):
        layer = 2 * pair
        wait_weights(layer, (0,))

        @pl.when(pair == 0)
        def _():
            start_weights(0, 1)
            for v in range(1, videos):
                pltpu.make_async_copy(x_ref.at[v], s_in.at[0, v], x_sem.at[v]).start()

        spatial(pair)
        wait_weights(layer + 1, range(len(weights)))

        @pl.when(pair < pairs - 1)
        def _():
            start_weights(layer + 2)

        temporal(pair)
        return carry

    lax.fori_loop(0, pairs, run_pair, 0)

    for v in range(videos):
        for h in range(halves):
            part = t_in.at[0, v, h, pl.ds(0, frames - f_loc)]
            for pair in range(pairs - 1):
                pltpu.make_async_copy(part, part, b_send.at[pair, v, h]).wait()
            for pair in range(pairs):
                pltpu.make_async_copy(part, part, ac_send.at[pair, v, h if v else 0]).wait()


def solution(mesh):
    n = mesh.shape["sp"]

    def local_stack(x, norms, w_qkv, w_out, w_up, w_down):
        videos, f_loc, patches, width = x.shape
        layers = w_qkv.shape[0]
        pairs = layers // 2
        head = w_qkv.shape[-1]
        hidden = w_up.shape[-1]
        frames, halves = f_loc * n, patches // n // SUB
        x = x.reshape(videos, f_loc, patches // SUB, SUB, width)
        w_qkv = w_qkv.transpose(0, 2, 3, 4, 1).reshape(layers, 3 * width, width)
        w_out = w_out.reshape(layers, width, width)
        any_space = pl.BlockSpec(memory_space=pl.ANY)
        y = pl.pallas_call(
            functools.partial(kernel, n, head),
            out_shape=pltpu.VMEM((videos, frames, halves, SUB, width), BF16),
            in_specs=[any_space, pl.BlockSpec(memory_space=pltpu.VMEM)] + [any_space] * 4,
            out_specs=pl.BlockSpec(memory_space=pltpu.VMEM),
            scratch_shapes=[
                pltpu.VMEM((layers, 3 * width, width), BF16),
                pltpu.VMEM((layers, width, width), BF16),
                pltpu.VMEM((layers, width, hidden), BF16),
                pltpu.VMEM((layers, hidden, width), BF16),
                pltpu.VMEM((pairs, videos, f_loc, patches // SUB, SUB, width), BF16),
                pltpu.VMEM((pairs, videos, f_loc, patches // SUB, SUB, width), BF16),
                pltpu.VMEM((pairs, videos, halves, frames, SUB, width), BF16),
                pltpu.VMEM((pairs - 1, videos, halves, frames, SUB, width), BF16),
                pltpu.VMEM((2, width // head, LANES, patches), BF16),
                pltpu.VMEM((2, patches, width), BF16),
                pltpu.VMEM((2, width, patches), BF16),
                pltpu.VMEM((2, width, patches), BF16),
                pltpu.VMEM((2, width // head, patches, patches), F32),
                pltpu.VMEM((2, patches, hidden), BF16),
                pltpu.VMEM((2, patches, width), BF16),
                pltpu.VMEM((2, patches, width), BF16),
                pltpu.VMEM((patches, width), BF16),
                pltpu.VMEM((patches, width), BF16),
                pltpu.VMEM((width // LANES, frames * SUB, LANES), F32),
                pltpu.VMEM((width // LANES, frames * SUB, LANES), F32),
                pltpu.VMEM((4 * frames, 4 * frames), F32),
                pltpu.SemaphoreType.DMA((layers, 4)),
                pltpu.SemaphoreType.DMA((videos,)),
                pltpu.SemaphoreType.DMA((pairs - 1, videos)),
                pltpu.SemaphoreType.DMA((pairs, videos, halves)),
                pltpu.SemaphoreType.DMA((pairs - 1, videos, halves)),
                pltpu.SemaphoreType.DMA((pairs, videos, halves)),
            ],
            compiler_params=pltpu.CompilerParams(collective_id=0, has_side_effects=True, vmem_limit_bytes=VMEM_BYTES),
            name="stack",
        )(x, norms, w_qkv, w_out, w_up, w_down)
        return y.reshape(videos, frames, halves * SUB, width)

    replicated = P()
    return jax.shard_map(local_stack, mesh=mesh, in_specs=(P('data', 'sp', None, None), replicated, replicated, replicated, replicated, replicated), out_specs=P('data', None, 'sp', None), check_vma=False)
```
